32 devices in a mesh: slab: 8 (over y, x, core), lev: 4 (over z).
Axes of the slice: x: 2, y: 2, z: 4, core: 2. Of those that a mesh axis runs over, the one named last changes fastest.
Arguments:
- ensemble: float32 [80, 16, 18432], P(None, 'lev', 'slab'), may hold values from -6 to 6
- obs_cell: int32 [2, 256], replicated, may hold values from 0 to 294911, as said below
- obs_value: float32 [2, 256], replicated, may hold values from -6 to 6
- obs_var: float32 [2, 256], replicated, may hold values from 0.3 to 3
- obs_frac: float32 [2, 256], replicated, may hold values from 0 to 1
- loc_column: bfloat16 [2, 256, 18432], P(None, 'lev', 'slab'), may hold values from 0 to 1
- loc_level: float32 [2, 256, 16], P(None, None, 'lev'), may hold values from 0.2 to 1
Outputs:
- analysis: float32 [80, 16, 18432], P(None, 'lev', 'slab')
- prior_mean: float32 [2, 256], replicated
The draws below stay inside these ranges and needn't reach their ends.
Inputs may be any that keep to these rules, and one draw needn't show every extreme that they name: `obs_cell`: in each block, every device's cells (a level band of 4 levels and a slab of 2304 columns) hold at least one observation, and one of them lies in the slab's last column.
All inputs are finite; a program needn't handle non-finite values.
Results may differ from the reference program's by a relative error of at most 0.0055.
Values may be sent and summed in bfloat16 or wider, within the bound.
No kernel may reach another device: no remote copies, remote signals or barrier semaphores. Data moves between devices by JAX's collectives and lax.ppermute only.
A program may use at most 64 MiB of HBM per device.

```python
import math
import jax
import jax.numpy as jnp
from jax import lax

MEM = 80
CL = 4
CC = 2304
NOBS = 256
BLOCKS = 2
NL = 16
NC = 18432


def draw_obs_cell(key, part):
    n_slabs = NC // CC
    n_bands = NL // CL
    owners = n_slabs * n_bands
    block_rows = []
    for block_index in range(BLOCKS):
        block_key = jax.random.fold_in(key, 101 + block_index)
        keys = jax.random.split(block_key, 6)
        owner_ids = jax.random.permutation(keys[0], owners).astype(jnp.int32)
        owner_slab = owner_ids % n_slabs
        owner_band = owner_ids // n_slabs
        owner_level = owner_band * CL + jax.random.randint(keys[1], (owners,), 0, CL, dtype=jnp.int32)
        owner_column = owner_slab * CC + CC - 1
        extra = NOBS - owners
        rest_level = jax.random.randint(keys[2], (extra,), 0, NL, dtype=jnp.int32)
        slab_one = jax.random.randint(keys[3], (extra,), 0, n_slabs, dtype=jnp.int32)
        slab_two = jax.random.randint(keys[4], (extra,), 0, n_slabs, dtype=jnp.int32)
        rest_slab = slab_one * slab_two // n_slabs
        rest_column = rest_slab * CC + jax.random.randint(keys[5], (extra,), 0, CC, dtype=jnp.int32)
        levels_all = jnp.concatenate([owner_level, rest_level])
        columns_all = jnp.concatenate([owner_column, rest_column])
        block_rows.append((levels_all * NC + columns_all).astype(jnp.int32))
    return jnp.stack(block_rows)


def steps_of(own_key, dims, cuts, smallest, largest):
    def one(position, shards_of):
        steps = jax.random.uniform(jax.random.fold_in(jax.random.fold_in(own_key, 6), position), (shards_of,), jnp.float32, smallest / len(cuts), largest / len(cuts))
        return jnp.repeat(jnp.exp(steps), dims[position] // shards_of).reshape((-1,) + (1,) * (len(dims) - position - 1))

    factor_of = one(*cuts[0])
    for cut in cuts[1:]:
        factor_of = factor_of * one(*cut)
    return factor_of


def scatter_about(key, shape, scale, reach, cuts=(), kind=jnp.bfloat16):
    gain = steps_of(key, shape, cuts, -0.22, 0.18) if cuts else 1.0
    array = jax.random.normal(key, shape, jnp.float32) * scale * gain
    return jnp.minimum(jnp.maximum(array, -reach), reach).astype(kind)


def setup_inputs(seed: int = 0) -> dict:
    seeds = jax.random.split(jax.random.key(seed), 8)
    ensemble = scatter_about(seeds[0], (MEM, NL, NC), 1.0, 6.0, ((1, 4), (2, 8)), jnp.float32)
    obs_cell = draw_obs_cell(jax.random.fold_in(seeds[7], 71), 0)
    obs_value = scatter_about(seeds[2], (BLOCKS, NOBS), 1.5, 6.0, (), jnp.float32)
    obs_var = jnp.clip(jnp.exp(jax.random.uniform(seeds[3], (BLOCKS, NOBS), jnp.float32, math.log(0.3), math.log(3.0))), 0.3, 3.0)
    obs_frac = jnp.clip(jax.random.uniform(seeds[4], (BLOCKS, NOBS), jnp.float32, 0.0, 1.0), 0.0, 1.0)
    loc_column = jnp.clip(1.0 * jax.random.uniform(seeds[5], (BLOCKS, NOBS, NC), jnp.float32) ** steps_of(seeds[5], (BLOCKS, NOBS, NC), ((1, 4), (2, 8)), -0.2, 0.2), 0.0, 1.0).astype(jnp.bfloat16)
    loc_level = jnp.clip(0.2 + 0.8 * jax.random.uniform(seeds[6], (BLOCKS, NOBS, NL), jnp.float32) ** steps_of(seeds[6], (BLOCKS, NOBS, NL), ((2, 4),), -0.2, 0.2), 0.2, 1.0)
    return dict(ensemble=ensemble, obs_cell=obs_cell, obs_value=obs_value, obs_var=obs_var, obs_frac=obs_frac, loc_column=loc_column, loc_level=loc_level)


def obs_stats(prior_obs, obs_val, variance):
    members = prior_obs.shape[1]
    obs_mean = lax.optimization_barrier(jnp.mean(prior_obs, axis=1))
    deviation = prior_obs - obs_mean[:, None]
    spread = lax.optimization_barrier(jnp.sum(deviation * deviation, axis=1)) / (members - 1.0)
    total_var = spread + variance
    shrink = 1.0 / (1.0 + jnp.sqrt(variance / total_var))
    gain_rows = ((obs_val - obs_mean)[:, None] - deviation * shrink[:, None]) / (total_var * (members - 1.0))[:, None]
    return (obs_mean, deviation.astype(jnp.bfloat16), gain_rows.astype(jnp.bfloat16))

def reference(ensemble, obs_cell, obs_value, obs_var, obs_frac, loc_column, loc_level):
    current = ensemble
    prior_means = []
    for block_index in range(BLOCKS):
        obs_cells = obs_cell[block_index]
        obs_level = obs_cells // NC
        obs_column = obs_cells % NC
        next_column = (obs_column + 1) % NC
        flattened = current.reshape(MEM, NL * NC)
        first_val = jnp.take(flattened, obs_level * NC + obs_column, axis=1)
        second = jnp.take(flattened, obs_level * NC + next_column, axis=1)
        fraction = obs_frac[block_index]
        prior_obs = ((1.0 - fraction)[None, :] * first_val + fraction[None, :] * second).T
        obs_mean, dev_b, gain_b = obs_stats(prior_obs, obs_value[block_index], obs_var[block_index])
        prior_means.append(obs_mean)
        centred = (current - lax.optimization_barrier(jnp.mean(current, axis=0))).astype(jnp.bfloat16)
        col_weights = loc_column[block_index]
        lev_weights = loc_level[block_index]

        def level_step(level_index):
            level_slab = lax.dynamic_index_in_dim(centred, level_index, 1, keepdims=False)
            level_loc = lax.dynamic_index_in_dim(lev_weights, level_index, 1, keepdims=False)
            cross_cov = jnp.dot(dev_b, level_slab, preferred_element_type=jnp.float32)
            mixed_rows = (level_loc[:, None] * col_weights.astype(jnp.float32) * cross_cov).astype(jnp.bfloat16)
            return jnp.dot(gain_b.T, mixed_rows, preferred_element_type=jnp.float32)
        increment = lax.map(level_step, jnp.arange(NL, dtype=jnp.int32))
        current = current + jnp.transpose(increment, (1, 0, 2))
    return (current, jnp.stack(prior_means))
```

```python
import functools

import jax
import jax.numpy as jnp
from jax import lax
from jax.experimental import pallas as pl
from jax.experimental.pallas import tpu as pltpu
from jax.sharding import PartitionSpec as P

LANES = 128
CELL_BITS = 16


def swap(value, axis, bit):
    size = lax.axis_size(axis)
    return lax.ppermute(value, axis, [(i, i ^ bit) for i in range(size)])


def add_over(value, axes):
    for axis in axes:
        size = lax.axis_size(axis)
        if size & (size - 1):
            value = lax.psum(value, axis)
            continue
        bit = 1
        while bit < size:
            value = value + swap(value, axis, bit)
            bit *= 2
    return value


def rows_over(own, axis):
    size = lax.axis_size(axis)
    shards = {0: own}
    bit = size // 2
    order = sorted(range(1, size), key=lambda p: (bin(p).count("1"), -p))
    for p in order:
        low = p & -p
        shards[p] = swap(shards[p ^ low], axis, low)
    return [shards[p] for p in range(size)]


def list_owned(key_ref, list_ref, count):
    def step(o, found):
        key = key_ref[0, o]
        list_ref[found] = o
        return found + (key >= 0).astype(jnp.int32)

    return lax.fori_loop(0, count, step, jnp.int32(0), unroll=8)


def gather_priors(key_ref, frac_ref, list_ref, found, source_ref, out_ref):
    members = out_ref.shape[0]
    slab_cols = source_ref.shape[2]
    lane = lax.broadcasted_iota(jnp.int32, (members, LANES), 1)
    out_ref[...] = jnp.zeros(out_ref.shape, jnp.float32)

    def step(i, carry):
        o = list_ref[i]
        key = key_ref[0, o]
        fraction = frac_ref[0, o]
        row = key >> CELL_BITS
        col = (key & ((1 << CELL_BITS) - 1)) - 1
        first = jnp.maximum(col, 0)
        second = jnp.minimum(col + 1, slab_cols - 1)
        weight_first = jnp.where(col >= 0, 1.0 - fraction, 0.0)
        weight_second = jnp.where(col + 1 < slab_cols, fraction, 0.0)
        slot = o & (LANES - 1)

        def picked(c):
            tile = source_ref[row, :, pl.ds(pl.multiple_of((c >> 7) * LANES, LANES), LANES)]
            return pltpu.roll(tile, (slot - c) & (LANES - 1), 1)

        value = weight_first * picked(first) + weight_second * picked(second)
        where_out = pl.ds(pl.multiple_of((o >> 7) * LANES, LANES), LANES)
        out_ref[:, where_out] = jnp.where(lane == slot, value, out_ref[:, where_out])
        return carry

    lax.fori_loop(0, found, step, 0)


def load_levels(ens_ref, cur_ref, sems):
    return [
        pltpu.make_async_copy(ens_ref.at[:, l, :], cur_ref.at[l], sems.at[l])
        for l in range(cur_ref.shape[0])
    ]


def prior_kernel(key_ref, frac_ref, ens_ref, out_ref, cur_ref, list_ref, sems):
    copies = load_levels(ens_ref, cur_ref, sems)
    for copy in copies:
        copy.start()
    found = list_owned(key_ref, list_ref, key_ref.shape[1])
    for copy in copies:
        copy.wait()
    gather_priors(key_ref, frac_ref, list_ref, found, cur_ref, out_ref)


def regroup(value, lev_index, groups):
    total = value.shape[1]
    lane = lax.broadcasted_iota(jnp.int32, value.shape, 1)
    bit = 1
    while bit < groups:
        span = (total // groups) * bit
        other = jnp.where(
            (lane & span) != 0, pltpu.roll(value, span, 1), pltpu.roll(value, total - span, 1)
        )
        value = jnp.where((lev_index & bit) != 0, other, value)
        bit *= 2
    return value


def observe(lev_index, groups, prior_ref, value_ref, var_ref, level_ref, mean_ref, dev_ref, gain_ref, level_b_ref):
    prior = prior_ref[...]
    members, n_obs = prior.shape
    lev_rows = level_ref.shape[1]
    variance = var_ref[0]
    obs_mean = jnp.sum(prior, axis=0, keepdims=True) / members
    mean_ref[...] = obs_mean
    deviation = prior - obs_mean
    spread = jnp.sum(deviation * deviation, axis=0, keepdims=True) / (members - 1.0)
    total_var = spread + variance
    shrink = 1.0 / (1.0 + jnp.sqrt(variance / total_var))
    gain = ((value_ref[0] - obs_mean) - deviation * shrink) / (total_var * (members - 1.0))
    gain_ref[...] = regroup(gain, lev_index, groups).astype(jnp.bfloat16)
    pad = jnp.zeros((LANES - members, n_obs), jnp.float32)
    dev_all = jnp.concatenate([regroup(deviation, lev_index, groups), pad], axis=0)
    dev_ref[...] = dev_all.T[:, :members].astype(jnp.bfloat16)
    level_all = jnp.concatenate(
        [regroup(level_ref[0], lev_index, groups), jnp.zeros((LANES - lev_rows, n_obs), jnp.float32)], axis=0
    ).T
    for l in range(lev_rows):
        level_b_ref[l] = jnp.broadcast_to(level_all[:, l : l + 1], (n_obs, LANES))


def regress(cur_of, put, shards, dev_ref, gain_ref, level_b_ref, l, slab_cols, width):
    dev = dev_ref[...]
    gain = gain_ref[...]
    reps = width // LANES

    def step(i, carry):
        cols = pl.ds(pl.multiple_of(i * width, width), width)
        field = cur_of(cols)
        members = field.shape[0]
        centred = (field - jnp.sum(field, axis=0, keepdims=True) / members).astype(jnp.bfloat16)
        cross = jnp.dot(dev, centred, preferred_element_type=jnp.float32)
        weights = jnp.concatenate([s[0, :, cols] if len(s.shape) == 3 else s[:, cols] for s in shards], axis=0)
        level = jnp.concatenate([level_b_ref[l]] * reps, axis=1)
        mixed = ((level * weights.astype(jnp.float32)) * cross).astype(jnp.bfloat16)
        put(cols, field + jnp.dot(gain, mixed, preferred_element_type=jnp.float32))
        return carry

    lax.fori_loop(0, slab_cols // width, step, 0)


def first_kernel(groups, width, lev_ref, key_ref, frac_ref, prior_ref, value_ref, var_ref, level_ref, ens_ref, *rest):
    shards = rest[:groups]
    cur_out, mean_ref, next_ref, cur_ref, dev_ref, gain_ref, level_b_ref, list_ref, sems = rest[groups:]
    lev_rows, members, slab_cols = cur_ref.shape
    copies = load_levels(ens_ref, cur_ref, sems)
    for copy in copies:
        copy.start()
    found = list_owned(key_ref, list_ref, key_ref.shape[1])
    observe(lev_ref[0], groups, prior_ref, value_ref, var_ref, level_ref, mean_ref, dev_ref, gain_ref, level_b_ref)
    for l in range(lev_rows):
        copies[l].wait()

        def put(cols, value, l=l):
            cur_out[l, :, cols] = value

        regress(lambda cols, l=l: cur_ref[l, :, cols], put, shards, dev_ref, gain_ref, level_b_ref, l, slab_cols, width)
    gather_priors(key_ref, frac_ref, list_ref, found, cur_out, next_ref)


def last_kernel(groups, width, lev_ref, prior_ref, value_ref, var_ref, level_ref, cur_ref, *rest):
    shards = rest[:groups]
    ens_out, mean_ref, buf_ref, dev_ref, gain_ref, level_b_ref, sems = rest[groups:]
    lev_rows, members, slab_cols = cur_ref.shape
    observe(lev_ref[0], groups, prior_ref, value_ref, var_ref, level_ref, mean_ref, dev_ref, gain_ref, level_b_ref)
    copies = []
    for l in range(lev_rows):

        def put(cols, value, l=l):
            buf_ref[l, :, cols] = value

        regress(lambda cols, l=l: cur_ref[l, :, cols], put, shards, dev_ref, gain_ref, level_b_ref, l, slab_cols, width)
        copies.append(pltpu.make_async_copy(buf_ref.at[l], ens_out.at[:, l, :], sems.at[l]))
        copies[l].start()
    for copy in copies:
        copy.wait()


def smem_row(b, n_obs):
    return pl.BlockSpec((1, n_obs), lambda *_: (b, 0), memory_space=pltpu.SMEM)


def on_device(ensemble, obs_cell, obs_value, obs_var, obs_frac, loc_column, loc_level):
    members, lev_rows, slab_cols = ensemble.shape
    n_blocks, n_obs = obs_cell.shape
    shard_rows = loc_column.shape[1]
    groups = lax.axis_size("lev")
    n_slabs = lax.axis_size("slab")
    total_cols = slab_cols * n_slabs
    width = 256 if slab_cols % 256 == 0 else LANES
    lev_index = lax.axis_index("lev")

    local_row = obs_cell // total_cols - lev_index * lev_rows
    local_col = (obs_cell % total_cols - lax.axis_index("slab") * slab_cols + 1) % total_cols
    owned = (local_row >= 0) & (local_row < lev_rows) & (local_col <= slab_cols)
    keys = jnp.where(owned, (local_row << CELL_BITS) + local_col, -1).reshape(n_blocks, 1, n_obs)
    fracs = obs_frac.reshape(n_blocks, 1, n_obs)
    values = obs_value.reshape(n_blocks, 1, n_obs)
    variances = obs_var.reshape(n_blocks, 1, n_obs)
    levels = loc_level.transpose(0, 2, 1)
    lev_scalar = lev_index.reshape(1).astype(jnp.int32)

    smem = pl.BlockSpec(memory_space=pltpu.SMEM)
    vmem = pl.BlockSpec(memory_space=pltpu.VMEM)
    hbm = pl.BlockSpec(memory_space=pl.ANY)
    f32 = jnp.float32
    field = jax.ShapeDtypeStruct((lev_rows, members, slab_cols), f32)
    row = jax.ShapeDtypeStruct((1, n_obs), f32)
    rows = jax.ShapeDtypeStruct((members, n_obs), f32)
    field_scratch = pltpu.VMEM((lev_rows, members, slab_cols), f32)
    work = [
        pltpu.VMEM((n_obs, members), jnp.bfloat16),
        pltpu.VMEM((members, n_obs), jnp.bfloat16),
        pltpu.VMEM((lev_rows, n_obs, LANES), f32),
    ]
    own_list = pltpu.SMEM((n_obs,), jnp.int32)
    dma = pltpu.SemaphoreType.DMA((lev_rows,))

    shards = [rows_over(loc_column[b], "lev") for b in range(n_blocks)]

    prior = pl.pallas_call(
        prior_kernel,
        out_shape=rows,
        in_specs=[smem, smem, hbm],
        out_specs=vmem,
        scratch_shapes=[field_scratch, own_list, dma],
        name="cells",
    )(keys[0], fracs[0], ensemble)
    prior = add_over(prior, ("slab", "lev"))

    current, mean_first, prior_next = pl.pallas_call(
        functools.partial(first_kernel, groups, width),
        out_shape=(field, row, rows),
        in_specs=[smem, smem, smem, vmem, vmem, vmem, vmem, hbm] + [vmem] * groups,
        out_specs=(vmem, vmem, vmem),
        scratch_shapes=[field_scratch] + work + [own_list, dma],
        name="block_first",
    )(lev_scalar, keys[1], fracs[1], prior, values[:1], variances[:1], levels[:1], ensemble, *shards[0])
    prior_next = add_over(prior_next, ("slab", "lev"))

    analysis, mean_last = pl.pallas_call(
        functools.partial(last_kernel, groups, width),
        out_shape=(jax.ShapeDtypeStruct(ensemble.shape, f32), row),
        in_specs=[smem, vmem, vmem, vmem, vmem, vmem] + [vmem] * groups,
        out_specs=(hbm, vmem),
        scratch_shapes=[field_scratch] + work + [dma],
        name="block_last",
    )(lev_scalar, prior_next, values[1:], variances[1:], levels[1:], current, *shards[1])
    return (analysis, jnp.concatenate([mean_first, mean_last], axis=0))


def solution(mesh):
    in_specs = (
        P(None, "lev", "slab"),
        P(),
        P(),
        P(),
        P(),
        P(None, "lev", "slab"),
        P(None, None, "lev"),
    )
    out_specs = (P(None, "lev", "slab"), P())
    return jax.shard_map(
        on_device, mesh=mesh, in_specs=in_specs, out_specs=out_specs, check_vma=False
    )
```

```python
import functools

import jax
import jax.numpy as jnp
from jax import lax
from jax.experimental import pallas as pl
from jax.experimental.pallas import tpu as pltpu
from jax.sharding import PartitionSpec as P


LANES = 128
CELL_BITS = 16


def swap(value, axis, bit):
    size = lax.axis_size(axis)
    return lax.ppermute(value, axis, [(i, i ^ bit) for i in range(size)])


def rounds_of(axis, first_bit):
    size = lax.axis_size(axis)
    if size & (size - 1):
        raise ValueError("axis size")
    bit = first_bit
    while bit < size:
        if bit * 2 < size:
            yield axis, (bit, bit * 2, bit * 3)
        else:
            yield axis, (bit,)
        bit *= 4


def add_over(keep, send):
    half = keep + swap(send, "slab", 1)
    rounds = list(rounds_of("slab", 2)) + list(rounds_of("lev", 1))
    for axis, distances in rounds:
        half = sum([swap(half, axis, d) for d in distances], half)
    return half, swap(half, "slab", 1)


def rows_over(own, axis):
    size = lax.axis_size(axis)
    shards = {0: own}
    order = sorted(range(1, size), key=lambda p: (bin(p).count("1"), -p))
    for p in order:
        low = p & -p
        shards[p] = swap(shards[p ^ low], axis, low)
    return [shards[p] for p in range(1, size)]


def list_owned(key_ref, list_ref, b):
    def step(o, found):
        list_ref[found] = o
        return found + (key_ref[b, o] >= 0).astype(jnp.int32)

    return lax.fori_loop(0, key_ref.shape[1], step, jnp.int32(0), unroll=8)


def gather_priors(key_ref, frac_ref, list_ref, b, found, source_ref, sum_ref):
    members = sum_ref.shape[0]
    slab_cols = source_ref.shape[2]
    lane = lax.broadcasted_iota(jnp.int32, (members, LANES), 1)
    sum_ref[...] = jnp.zeros(sum_ref.shape, jnp.float32)

    def step(i, carry):
        o = list_ref[i]
        key = key_ref[b, o]
        fraction = frac_ref[b, o]
        row = key >> CELL_BITS
        col = (key & ((1 << CELL_BITS) - 1)) - 1
        first = jnp.maximum(col, 0)
        second = jnp.minimum(col + 1, slab_cols - 1)
        weight_first = jnp.where(col >= 0, 1.0 - fraction, 0.0)
        weight_second = jnp.where(col + 1 < slab_cols, fraction, 0.0)
        slot = o & (LANES - 1)

        def picked(c):
            tile = source_ref[row, :, pl.ds(pl.multiple_of((c >> 7) * LANES, LANES), LANES)]
            return pltpu.roll(tile, (slot - c) & (LANES - 1), 1)

        value = weight_first * picked(first) + weight_second * picked(second)
        where_out = pl.ds(pl.multiple_of((o >> 7) * LANES, LANES), LANES)
        sum_ref[:, where_out] = jnp.where(lane == slot, value, sum_ref[:, where_out])
        return carry

    lax.fori_loop(0, found, step, 0)


def half_of(side, width):
    return pl.ds(pl.multiple_of(side * width, LANES), width)


def split_halves(side, sum_ref, keep_ref, send_ref):
    width = keep_ref.shape[1]
    keep_ref[...] = sum_ref[:, half_of(side, width)]
    send_ref[...] = sum_ref[:, half_of(1 - side, width)]


def load_levels(ens_ref, cur_ref, sems):
    return [
        pltpu.make_async_copy(ens_ref.at[:, l, :], cur_ref.at[l], sems.at[l])
        for l in range(cur_ref.shape[0])
    ]


def prior_kernel(place_ref, key_ref, frac_ref, ens_ref, keep_ref, send_ref, cur_ref, sum_ref, list_ref, sems):
    copies = load_levels(ens_ref, cur_ref, sems)
    for copy in copies:
        copy.start()
    found = list_owned(key_ref, list_ref, 0)
    for copy in copies:
        copy.wait()
    gather_priors(key_ref, frac_ref, list_ref, 0, found, cur_ref, sum_ref)
    split_halves(place_ref[1], sum_ref, keep_ref, send_ref)


def regroup(value, lev_index, groups):
    total = value.shape[1]
    lane = lax.broadcasted_iota(jnp.int32, value.shape, 1)
    bit = 1
    while bit < groups:
        span = (total // groups) * bit
        other = jnp.where(
            (lane & span) != 0, pltpu.roll(value, span, 1), pltpu.roll(value, total - span, 1)
        )
        value = jnp.where((lev_index & bit) != 0, other, value)
        bit *= 2
    return value


def observe(b, groups, place_ref, own_ref, other_ref, value_ref, var_ref, level_ref, mean_ref, work):
    sum_ref, dev_ref, gain_ref, level_b_ref = work
    lev_index, side = place_ref[0], place_ref[1]
    width = own_ref.shape[1]
    sum_ref[:, half_of(side, width)] = own_ref[...]
    sum_ref[:, half_of(1 - side, width)] = other_ref[...]
    prior = sum_ref[...]
    members, n_obs = prior.shape
    lev_rows = level_ref.shape[1]
    variance = var_ref[b : b + 1]
    obs_mean = jnp.sum(prior, axis=0, keepdims=True) / members
    mean_ref[...] = obs_mean
    deviation = prior - obs_mean
    spread = jnp.sum(deviation * deviation, axis=0, keepdims=True) / (members - 1.0)
    total_var = spread + variance
    shrink = 1.0 / (1.0 + jnp.sqrt(variance / total_var))
    gain = ((value_ref[b : b + 1] - obs_mean) - deviation * shrink) / (total_var * (members - 1.0))
    gain_ref[...] = regroup(gain, lev_index, groups).astype(jnp.bfloat16)
    pad = jnp.zeros((LANES - members, n_obs), jnp.float32)
    dev_all = jnp.concatenate([regroup(deviation, lev_index, groups), pad], axis=0)
    dev_ref[...] = dev_all.T[:, :members].astype(jnp.bfloat16)
    level_all = jnp.concatenate(
        [regroup(level_ref[b], lev_index, groups), jnp.zeros((LANES - lev_rows, n_obs), jnp.float32)], axis=0
    ).T
    for l in range(lev_rows):
        level_b_ref[l] = jnp.broadcast_to(level_all[:, l : l + 1], (n_obs, LANES))


def regress(field, shards, l, work):
    _, dev_ref, gain_ref, level_b_ref = work
    members, slab_cols = field.shape
    centred = (field - jnp.sum(field, axis=0, keepdims=True) / members).astype(jnp.bfloat16)
    cross = jnp.dot(dev_ref[...], centred, preferred_element_type=jnp.float32)
    weights = jnp.concatenate([s[...] for s in shards], axis=0)
    level = jnp.concatenate([level_b_ref[l]] * (slab_cols // LANES), axis=1)
    mixed = ((level * weights.astype(jnp.float32)) * cross).astype(jnp.bfloat16)
    return field + jnp.dot(gain_ref[...], mixed, preferred_element_type=jnp.float32)


def first_kernel(groups, place_ref, key_ref, frac_ref, own_ref, other_ref, value_ref, var_ref, level_ref, ens_ref, *rest):
    shards = [rest[0].at[0], *rest[1:groups]]
    cur_out, mean_ref, keep_ref, send_ref, cur_ref, sum_ref, dev_ref, gain_ref, level_b_ref, list_ref, sems = rest[groups:]
    work = (sum_ref, dev_ref, gain_ref, level_b_ref)
    lev_rows = cur_ref.shape[0]
    copies = load_levels(ens_ref, cur_ref, sems)
    for copy in copies:
        copy.start()
    found = list_owned(key_ref, list_ref, 1)
    observe(0, groups, place_ref, own_ref, other_ref, value_ref, var_ref, level_ref, mean_ref, work)
    for l in range(lev_rows):
        copies[l].wait()
        cur_out[l] = regress(cur_ref[l], shards, l, work)
    gather_priors(key_ref, frac_ref, list_ref, 1, found, cur_out, sum_ref)
    split_halves(place_ref[1], sum_ref, keep_ref, send_ref)


def last_kernel(groups, place_ref, own_ref, other_ref, value_ref, var_ref, level_ref, cur_ref, *rest):
    shards = [rest[0].at[1], *rest[1:groups]]
    ens_out, mean_ref, buf_ref, sum_ref, dev_ref, gain_ref, level_b_ref, sems = rest[groups:]
    work = (sum_ref, dev_ref, gain_ref, level_b_ref)
    lev_rows = cur_ref.shape[0]
    observe(1, groups, place_ref, own_ref, other_ref, value_ref, var_ref, level_ref, mean_ref, work)
    copies = []
    for l in range(lev_rows):
        buf_ref[l] = regress(cur_ref[l], shards, l, work)
        copies.append(pltpu.make_async_copy(buf_ref.at[l], ens_out.at[:, l, :], sems.at[l]))
        copies[l].start()
    for copy in copies:
        copy.wait()


def on_device(ensemble, obs_cell, obs_value, obs_var, obs_frac, loc_column, loc_level):
    members, lev_rows, slab_cols = ensemble.shape
    n_blocks, n_obs = obs_cell.shape
    groups = lax.axis_size("lev")
    total_cols = slab_cols * lax.axis_size("slab")
    lev_index = lax.axis_index("lev")
    slab_index = lax.axis_index("slab")

    local_row = obs_cell // total_cols - lev_index * lev_rows
    local_col = (obs_cell % total_cols - slab_index * slab_cols + 1) % total_cols
    owned = (local_row >= 0) & (local_row < lev_rows) & (local_col <= slab_cols)
    keys = jnp.where(owned, (local_row << CELL_BITS) + local_col, -1)
    levels = loc_level.transpose(0, 2, 1)
    place = jnp.stack([lev_index, slab_index & 1]).astype(jnp.int32)

    smem = pl.BlockSpec(memory_space=pltpu.SMEM)
    vmem = pl.BlockSpec(memory_space=pltpu.VMEM)
    hbm = pl.BlockSpec(memory_space=pl.ANY)
    f32 = jnp.float32
    field = jax.ShapeDtypeStruct((lev_rows, members, slab_cols), f32)
    row = jax.ShapeDtypeStruct((1, n_obs), f32)
    half = jax.ShapeDtypeStruct((members, n_obs // 2), f32)
    field_scratch = pltpu.VMEM((lev_rows, members, slab_cols), f32)
    sum_scratch = pltpu.VMEM((members, n_obs), f32)
    work = [
        sum_scratch,
        pltpu.VMEM((n_obs, members), jnp.bfloat16),
        pltpu.VMEM((members, n_obs), jnp.bfloat16),
        pltpu.VMEM((lev_rows, n_obs, LANES), f32),
    ]
    own_list = pltpu.SMEM((n_obs,), jnp.int32)
    dma = pltpu.SemaphoreType.DMA((lev_rows,))

    shards = [rows_over(loc_column[b], "lev") for b in range(n_blocks)]

    keep, send = pl.pallas_call(
        prior_kernel,
        out_shape=(half, half),
        in_specs=[smem, smem, smem, hbm],
        out_specs=(vmem, vmem),
        scratch_shapes=[field_scratch, sum_scratch, own_list, dma],
        name="cells",
    )(place, keys, obs_frac, ensemble)
    own, other = add_over(keep, send)

    current, mean_first, keep, send = pl.pallas_call(
        functools.partial(first_kernel, groups),
        out_shape=(field, row, half, half),
        in_specs=[smem, smem, smem, vmem, vmem, vmem, vmem, vmem, hbm, vmem] + [vmem] * (groups - 1),
        out_specs=(vmem, vmem, vmem, vmem),
        scratch_shapes=[field_scratch] + work + [own_list, dma],
        name="block_first",
    )(place, keys, obs_frac, own, other, obs_value, obs_var, levels, ensemble, loc_column, *shards[0])
    own, other = add_over(keep, send)

    analysis, mean_last = pl.pallas_call(
        functools.partial(last_kernel, groups),
        out_shape=(jax.ShapeDtypeStruct(ensemble.shape, f32), row),
        in_specs=[smem, vmem, vmem, vmem, vmem, vmem, vmem, vmem] + [vmem] * (groups - 1),
        out_specs=(hbm, vmem),
        scratch_shapes=[field_scratch] + work + [dma],
        name="block_last",
    )(place, own, other, obs_value, obs_var, levels, current, loc_column, *shards[1])
    return (analysis, jnp.concatenate([mean_first, mean_last], axis=0))


def solution(mesh):
    in_specs = (
        P(None, "lev", "slab"),
        P(),
        P(),
        P(),
        P(),
        P(None, "lev", "slab"),
        P(None, None, "lev"),
    )
    out_specs = (P(None, "lev", "slab"), P())
    return jax.shard_map(
        on_device, mesh=mesh, in_specs=in_specs, out_specs=out_specs, check_vma=False
    )
```

```python
import functools

import jax
import jax.numpy as jnp
from jax import lax
from jax.experimental import pallas as pl
from jax.experimental.pallas import tpu as pltpu
from jax.sharding import PartitionSpec as P


LANES = 128
CELL_BITS = 16
BATCH = 4


def swap(value, axis, bit):
    size = lax.axis_size(axis)
    return lax.ppermute(value, axis, [(i, i ^ bit) for i in range(size)])


def rounds_of(axis, first_bit):
    size = lax.axis_size(axis)
    if size & (size - 1):
        raise ValueError("axis size")
    bit = first_bit
    while bit < size:
        if bit * 2 < size:
            yield axis, (bit, bit * 2, bit * 3)
        else:
            yield axis, (bit,)
        bit *= 4


def add_over(keep, send):
    half = keep + swap(send, "slab", 1)
    rounds = list(rounds_of("slab", 2)) + list(rounds_of("lev", 1))
    for axis, distances in rounds:
        half = sum([swap(half, axis, d) for d in distances], half)
    return half, swap(half, "slab", 1)


def rows_over(own, axis):
    size = lax.axis_size(axis)
    shards = {0: own}
    order = sorted(range(1, size), key=lambda p: (bin(p).count("1"), -p))
    for p in order:
        low = p & -p
        shards[p] = swap(shards[p ^ low], axis, low)
    return [shards[p] for p in range(1, size)]


def key_copy(place_ref, cell_ref, key_ref, key_smem, sem, sizes):
    lev_rows, slab_cols, total_cols = sizes
    lev_index, slab_index = place_ref[0], place_ref[1]
    cell = cell_ref[...]
    edge = slab_index == 0
    lowest = jnp.where(edge, 1, 0)
    key = jnp.full(cell.shape, -1, jnp.int32)
    for r in range(lev_rows):
        col = cell - ((lev_index * lev_rows + r) * total_cols + slab_index * slab_cols - 1)
        key = jnp.where((col >= lowest) & (col <= slab_cols), col + (r << CELL_BITS), key)
        key = jnp.where((col == total_cols) & edge, r << CELL_BITS, key)
    key_ref[...] = key
    return pltpu.make_async_copy(key_ref, key_smem, sem)


def list_owned(key_ref, list_ref, b):
    def step(o, found):
        list_ref[found] = o
        return found + (key_ref[b, o] >= 0).astype(jnp.int32)

    found = lax.fori_loop(0, key_ref.shape[1], step, jnp.int32(0), unroll=16)
    for extra in range(BATCH - 1):
        list_ref[found + extra] = 0
    return found


def gather_priors(key_ref, frac_ref, list_ref, b, found, source_ref, sum_ref):
    members = sum_ref.shape[0]
    slab_cols = source_ref.shape[2]
    lane = lax.broadcasted_iota(jnp.int32, (members, LANES), 1)
    sum_ref[...] = jnp.zeros(sum_ref.shape, jnp.float32)

    def value_of(i):
        o = list_ref[i]
        key = key_ref[b, o]
        fraction = frac_ref[b, o]
        row = jnp.maximum(key, 0) >> CELL_BITS
        col = (jnp.maximum(key, 0) & ((1 << CELL_BITS) - 1)) - 1
        first = jnp.maximum(col, 0)
        second = jnp.minimum(col + 1, slab_cols - 1)
        real = i < found
        weight_first = jnp.where(real & (col >= 0), 1.0 - fraction, 0.0)
        weight_second = jnp.where(real & (col + 1 < slab_cols), fraction, 0.0)
        slot = o & (LANES - 1)

        def picked(c):
            tile = source_ref[row, :, pl.ds(pl.multiple_of((c >> 7) * LANES, LANES), LANES)]
            return pltpu.roll(tile, (slot - c) & (LANES - 1), 1)

        value = weight_first * picked(first) + weight_second * picked(second)
        return (o >> 7) * LANES, jnp.where(lane == slot, value, 0.0)

    def step(i, carry):
        batch = [value_of(i * BATCH + k) for k in range(BATCH)]
        for start, value in batch:
            where_out = pl.ds(pl.multiple_of(start, LANES), LANES)
            sum_ref[:, where_out] = sum_ref[:, where_out] + value
        return carry

    lax.fori_loop(0, (found + BATCH - 1) // BATCH, step, 0)


def half_of(side, width):
    return pl.ds(pl.multiple_of(side * width, LANES), width)


def split_halves(side, sum_ref, keep_ref, send_ref):
    width = keep_ref.shape[1]
    keep_ref[...] = sum_ref[:, half_of(side, width)]
    send_ref[...] = sum_ref[:, half_of(1 - side, width)]


def load_levels(ens_ref, cur_ref, sems):
    return [
        pltpu.make_async_copy(ens_ref.at[:, l, :], cur_ref.at[l], sems.at[l])
        for l in range(cur_ref.shape[0])
    ]


def prior_kernel(sizes, place_ref, frac_ref, cell_ref, ens_ref, keep_ref, send_ref, cur_ref, sum_ref, key_ref, key_smem, list_ref, sems, key_sem):
    copies = load_levels(ens_ref, cur_ref, sems)
    for copy in copies:
        copy.start()
    keys = key_copy(place_ref, cell_ref, key_ref, key_smem, key_sem, sizes)
    keys.start()
    keys.wait()
    found = list_owned(key_smem, list_ref, 0)
    for copy in copies:
        copy.wait()
    gather_priors(key_smem, frac_ref, list_ref, 0, found, cur_ref, sum_ref)
    split_halves(place_ref[1] & 1, sum_ref, keep_ref, send_ref)


def regroup(value, lev_index, groups):
    total = value.shape[1]
    lane = lax.broadcasted_iota(jnp.int32, value.shape, 1)
    bit = 1
    while bit < groups:
        span = (total // groups) * bit
        other = jnp.where(
            (lane & span) != 0, pltpu.roll(value, span, 1), pltpu.roll(value, total - span, 1)
        )
        value = jnp.where((lev_index & bit) != 0, other, value)
        bit *= 2
    return value


def observe(b, groups, place_ref, own_ref, other_ref, value_ref, var_ref, level_ref, work):
    sum_ref, dev_ref, gain_ref, level_b_ref = work
    lev_index, side = place_ref[0], place_ref[1] & 1
    width = own_ref.shape[1]
    sum_ref[:, half_of(side, width)] = own_ref[...]
    sum_ref[:, half_of(1 - side, width)] = other_ref[...]
    prior = sum_ref[...]
    members, n_obs = prior.shape
    lev_rows = level_ref.shape[1]
    variance = var_ref[b : b + 1]
    obs_mean = jnp.sum(prior, axis=0, keepdims=True) / members
    deviation = prior - obs_mean
    spread = jnp.sum(deviation * deviation, axis=0, keepdims=True) / (members - 1.0)
    total_var = spread + variance
    shrink = 1.0 / (1.0 + jnp.sqrt(variance / total_var))
    gain = ((value_ref[b : b + 1] - obs_mean) - deviation * shrink) / (total_var * (members - 1.0))
    gain_ref[...] = regroup(gain, lev_index, groups).astype(jnp.bfloat16)
    pad = jnp.zeros((LANES - members, n_obs), jnp.float32)
    dev_all = jnp.concatenate([regroup(deviation, lev_index, groups), pad], axis=0)
    dev_ref[...] = dev_all.T[:, :members].astype(jnp.bfloat16)
    level_all = jnp.concatenate(
        [regroup(level_ref[b], lev_index, groups), jnp.zeros((LANES - lev_rows, n_obs), jnp.float32)], axis=0
    ).T
    for l in range(lev_rows):
        level_b_ref[l] = jnp.broadcast_to(level_all[:, l : l + 1], (n_obs, LANES))
    return obs_mean


def regress(field, rows_ref, l, work):
    _, dev_ref, gain_ref, level_b_ref = work
    members, slab_cols = field.shape
    centred = (field - jnp.sum(field, axis=0, keepdims=True) / members).astype(jnp.bfloat16)
    cross = jnp.dot(dev_ref[...], centred, preferred_element_type=jnp.float32)
    level = jnp.concatenate([level_b_ref[l]] * (slab_cols // LANES), axis=1)
    mixed = ((level * rows_ref[...].astype(jnp.float32)) * cross).astype(jnp.bfloat16)
    return field + jnp.dot(gain_ref[...], mixed, preferred_element_type=jnp.float32)


def load_rows(b, shards, rows_ref, sems):
    own, *rest = shards
    count = own.shape[1]
    return [
        pltpu.make_async_copy(own.at[b] if p == 0 else rest[p - 1], rows_ref.at[pl.ds(p * count, count)], sems.at[p])
        for p in range(len(shards))
    ]


def first_kernel(groups, sizes, place_ref, frac_ref, cell_ref, own_ref, other_ref, value_ref, var_ref, level_ref, ens_ref, *rest):
    shards = rest[:groups]
    cur_out, mean_ref, keep_ref, send_ref, cur_ref, rows_ref, *work, key_ref, key_smem, list_ref, sems, row_sems, key_sem = rest[groups:]
    lev_rows = cur_ref.shape[0]
    keys = key_copy(place_ref, cell_ref, key_ref, key_smem, key_sem, sizes)
    keys.start()
    copies = load_levels(ens_ref, cur_ref, sems)
    rows = load_rows(0, shards, rows_ref, row_sems)
    for copy in copies[:1] + rows + copies[1:]:
        copy.start()
    mean_ref[...] = observe(0, groups, place_ref, own_ref, other_ref, value_ref, var_ref, level_ref, work)
    keys.wait()
    found = list_owned(key_smem, list_ref, 1)
    for copy in rows:
        copy.wait()
    for l in range(lev_rows):
        copies[l].wait()
        cur_out[l] = regress(cur_ref[l], rows_ref, l, work)
    gather_priors(key_smem, frac_ref, list_ref, 1, found, cur_out, work[0])
    split_halves(place_ref[1] & 1, work[0], keep_ref, send_ref)


def last_kernel(groups, place_ref, own_ref, other_ref, value_ref, var_ref, level_ref, mean_in, cur_in, *rest):
    shards = rest[:groups]
    ens_out, mean_ref, cur_ref, rows_ref, buf_ref, *work, sems, row_sems = rest[groups:]
    lev_rows = cur_ref.shape[0]
    copies = [pltpu.make_async_copy(cur_in.at[l], cur_ref.at[l], sems.at[l]) for l in range(lev_rows)]
    rows = load_rows(1, shards, rows_ref, row_sems)
    for copy in copies[:1] + rows + copies[1:]:
        copy.start()
    mean_ref[0:1] = mean_in[...]
    mean_ref[1:2] = observe(1, groups, place_ref, own_ref, other_ref, value_ref, var_ref, level_ref, work)
    for copy in rows:
        copy.wait()
    stores = []
    for l in range(lev_rows):
        copies[l].wait()
        buf_ref[l] = regress(cur_ref[l], rows_ref, l, work)
        stores.append(pltpu.make_async_copy(buf_ref.at[l], ens_out.at[:, l, :], sems.at[l]))
        stores[l].start()
    for store in stores:
        store.wait()


def with_place(kernel):
    def run(lev_ref, slab_ref, *refs):
        kernel((lev_ref[0], slab_ref[0]), *refs)

    return run


def on_device(ensemble, obs_cell, obs_value, obs_var, obs_frac, loc_column, loc_level):
    members, lev_rows, slab_cols = ensemble.shape
    n_blocks, n_obs = obs_cell.shape
    groups = lax.axis_size("lev")
    sizes = (lev_rows, slab_cols, slab_cols * lax.axis_size("slab"))
    place = [lax.axis_index(axis).reshape(1).astype(jnp.int32) for axis in ("lev", "slab")]
    levels = loc_level.transpose(0, 2, 1)

    smem = pl.BlockSpec(memory_space=pltpu.SMEM)
    vmem = pl.BlockSpec(memory_space=pltpu.VMEM)
    hbm = pl.BlockSpec(memory_space=pl.ANY)
    f32 = jnp.float32
    field = jax.ShapeDtypeStruct((lev_rows, members, slab_cols), f32)
    row = jax.ShapeDtypeStruct((1, n_obs), f32)
    half = jax.ShapeDtypeStruct((members, n_obs // 2), f32)
    field_scratch = pltpu.VMEM((lev_rows, members, slab_cols), f32)
    rows_scratch = pltpu.VMEM((n_obs, slab_cols), jnp.bfloat16)
    sum_scratch = pltpu.VMEM((members, n_obs), f32)
    work = [
        sum_scratch,
        pltpu.VMEM((n_obs, members), jnp.bfloat16),
        pltpu.VMEM((members, n_obs), jnp.bfloat16),
        pltpu.VMEM((lev_rows, n_obs, LANES), f32),
    ]
    own = [
        pltpu.VMEM((n_blocks, n_obs), jnp.int32),
        pltpu.SMEM((n_blocks, n_obs), jnp.int32),
        pltpu.SMEM((n_obs + BATCH,), jnp.int32),
    ]
    dma = pltpu.SemaphoreType.DMA((lev_rows,))
    row_dma = pltpu.SemaphoreType.DMA((groups,))
    one_dma = pltpu.SemaphoreType.DMA

    shards = [rows_over(loc_column[0], "lev")]

    keep, send = pl.pallas_call(
        with_place(functools.partial(prior_kernel, sizes)),
        out_shape=(half, half),
        in_specs=[smem, smem, smem, vmem, hbm],
        out_specs=(vmem, vmem),
        scratch_shapes=[field_scratch, sum_scratch] + own + [dma, one_dma],
        name="cells",
    )(*place, obs_frac, obs_cell, ensemble)
    later_rows, keep = lax.optimization_barrier((loc_column, keep))
    shards.append(rows_over(later_rows[1], "lev"))
    ours, theirs = add_over(keep, send)

    current, mean_first, keep, send = pl.pallas_call(
        with_place(functools.partial(first_kernel, groups, sizes)),
        out_shape=(field, row, half, half),
        in_specs=[smem, smem, smem] + [vmem] * 6 + [hbm] * (1 + groups),
        out_specs=(vmem, vmem, vmem, vmem),
        scratch_shapes=[field_scratch, rows_scratch] + work + own + [dma, row_dma, one_dma],
        name="block_first",
    )(*place, obs_frac, obs_cell, ours, theirs, obs_value, obs_var, levels, ensemble, loc_column, *shards[0])
    ours, theirs = add_over(keep, send)

    analysis, mean = pl.pallas_call(
        with_place(functools.partial(last_kernel, groups)),
        out_shape=(jax.ShapeDtypeStruct(ensemble.shape, f32), jax.ShapeDtypeStruct((n_blocks, n_obs), f32)),
        in_specs=[smem, smem] + [vmem] * 6 + [hbm] * (1 + groups),
        out_specs=(hbm, vmem),
        scratch_shapes=[field_scratch, rows_scratch, field_scratch] + work + [dma, row_dma],
        name="block_last",
    )(*place, ours, theirs, obs_value, obs_var, levels, mean_first, current, loc_column, *shards[1])
    return (analysis, mean)


def solution(mesh):
    in_specs = (
        P(None, "lev", "slab"),
        P(),
        P(),
        P(),
        P(),
        P(None, "lev", "slab"),
        P(None, None, "lev"),
    )
    out_specs = (P(None, "lev", "slab"), P())
    return jax.shard_map(
        on_device, mesh=mesh, in_specs=in_specs, out_specs=out_specs, check_vma=False
    )
```

```python
import functools

import jax
import jax.numpy as jnp
from jax import lax
from jax.experimental import pallas as pl
from jax.experimental.pallas import tpu as pltpu
from jax.sharding import PartitionSpec as P


LANES = 128
CELL_BITS = 16
BATCH = 4
KERNEL_VMEM = 32 * 1024 * 1024


def swap(value, axis, bit):
    size = lax.axis_size(axis)
    return lax.ppermute(value, axis, [(i, i ^ bit) for i in range(size)])


def rounds_of(axis, first_bit):
    size = lax.axis_size(axis)
    if size & (size - 1):
        raise ValueError("axis size")
    bit = first_bit
    while bit < size:
        if bit * 2 < size:
            yield axis, (bit, bit * 2, bit * 3)
        else:
            yield axis, (bit,)
        bit *= 4


def add_over(keep, send):
    half = keep + swap(send, "slab", 1)
    rounds = list(rounds_of("lev", 1)) + list(rounds_of("slab", 2))
    for axis, distances in rounds:
        half = sum([swap(half, axis, d) for d in distances], half)
    return half, swap(half, "slab", 1)


def rows_over(own, axis):
    size = lax.axis_size(axis)
    shards = {0: own}
    order = sorted(range(1, size), key=lambda p: (bin(p).count("1"), -p))
    for p in order:
        low = p & -p
        shards[p] = swap(shards[p ^ low], axis, low)
    return [shards[p] for p in range(1, size)]


def key_copy(place_ref, cell_ref, key_ref, key_smem, sem, sizes):
    lev_rows, slab_cols, total_cols = sizes
    lev_index, slab_index = place_ref[0], place_ref[1]
    cell = cell_ref[...]
    edge = slab_index == 0
    lowest = jnp.where(edge, 1, 0)
    key = jnp.full(cell.shape, -1, jnp.int32)
    for r in range(lev_rows):
        col = cell - ((lev_index * lev_rows + r) * total_cols + slab_index * slab_cols - 1)
        key = jnp.where((col >= lowest) & (col <= slab_cols), col + (r << CELL_BITS), key)
        key = jnp.where((col == total_cols) & edge, r << CELL_BITS, key)
    key_ref[...] = key
    return pltpu.make_async_copy(key_ref, key_smem, sem)


def list_owned(key_ref, list_ref, b):
    def step(o, found):
        list_ref[found] = o
        return found + (key_ref[b, o] >= 0).astype(jnp.int32)

    found = lax.fori_loop(0, key_ref.shape[1], step, jnp.int32(0), unroll=16)
    for extra in range(BATCH - 1):
        list_ref[found + extra] = 0
    return found


def gather_priors(key_ref, frac_ref, list_ref, b, found, source_ref, sum_ref):
    members = sum_ref.shape[0]
    slab_cols = source_ref.shape[2]
    lane = lax.broadcasted_iota(jnp.int32, (members, LANES), 1)
    sum_ref[...] = jnp.zeros(sum_ref.shape, jnp.float32)

    def value_of(i):
        o = list_ref[i]
        key = key_ref[b, o]
        fraction = frac_ref[b, o]
        row = jnp.maximum(key, 0) >> CELL_BITS
        col = (jnp.maximum(key, 0) & ((1 << CELL_BITS) - 1)) - 1
        first = jnp.maximum(col, 0)
        second = jnp.minimum(col + 1, slab_cols - 1)
        real = i < found
        weight_first = jnp.where(real & (col >= 0), 1.0 - fraction, 0.0)
        weight_second = jnp.where(real & (col + 1 < slab_cols), fraction, 0.0)
        slot = o & (LANES - 1)

        def picked(c):
            tile = source_ref[row, :, pl.ds(pl.multiple_of((c >> 7) * LANES, LANES), LANES)]
            return pltpu.roll(tile, (slot - c) & (LANES - 1), 1)

        value = weight_first * picked(first) + weight_second * picked(second)
        return (o >> 7) * LANES, jnp.where(lane == slot, value, 0.0)

    def step(i, carry):
        batch = [value_of(i * BATCH + k) for k in range(BATCH)]
        for start, value in batch:
            where_out = pl.ds(pl.multiple_of(start, LANES), LANES)
            sum_ref[:, where_out] = sum_ref[:, where_out] + value
        return carry

    lax.fori_loop(0, (found + BATCH - 1) // BATCH, step, 0)


def half_of(side, width):
    return pl.ds(pl.multiple_of(side * width, LANES), width)


def split_halves(side, sum_ref, keep_ref, send_ref):
    width = keep_ref.shape[1]
    keep_ref[...] = sum_ref[:, half_of(side, width)]
    send_ref[...] = sum_ref[:, half_of(1 - side, width)]


def load_levels(ens_ref, cur_ref, sems):
    return [
        pltpu.make_async_copy(ens_ref.at[:, l, :], cur_ref.at[l], sems.at[l])
        for l in range(cur_ref.shape[0])
    ]


def prior_kernel(sizes, place_ref, frac_ref, cell_ref, ens_ref, keep_ref, send_ref, cur_ref, sum_ref, key_ref, key_smem, list_ref, sems, key_sem):
    copies = load_levels(ens_ref, cur_ref, sems)
    for copy in copies:
        copy.start()
    keys = key_copy(place_ref, cell_ref, key_ref, key_smem, key_sem, sizes)
    keys.start()
    keys.wait()
    found = list_owned(key_smem, list_ref, 0)
    for copy in copies:
        copy.wait()
    gather_priors(key_smem, frac_ref, list_ref, 0, found, cur_ref, sum_ref)
    split_halves(place_ref[1] & 1, sum_ref, keep_ref, send_ref)


def regroup(value, lev_index, groups):
    total = value.shape[1]
    lane = lax.broadcasted_iota(jnp.int32, value.shape, 1)
    bit = 1
    while bit < groups:
        span = (total // groups) * bit
        other = jnp.where(
            (lane & span) != 0, pltpu.roll(value, span, 1), pltpu.roll(value, total - span, 1)
        )
        value = jnp.where((lev_index & bit) != 0, other, value)
        bit *= 2
    return value


def observe(b, groups, place_ref, own_ref, other_ref, value_ref, var_ref, level_ref, work):
    sum_ref, dev_ref, gain_ref, level_b_ref = work
    lev_index, side = place_ref[0], place_ref[1] & 1
    width = own_ref.shape[1]
    sum_ref[:, half_of(side, width)] = own_ref[...]
    sum_ref[:, half_of(1 - side, width)] = other_ref[...]
    prior = sum_ref[...]
    members, n_obs = prior.shape
    lev_rows = level_ref.shape[1]
    variance = var_ref[b : b + 1]
    obs_mean = jnp.sum(prior, axis=0, keepdims=True) / members
    deviation = prior - obs_mean
    spread = jnp.sum(deviation * deviation, axis=0, keepdims=True) / (members - 1.0)
    total_var = spread + variance
    shrink = 1.0 / (1.0 + jnp.sqrt(variance / total_var))
    gain = ((value_ref[b : b + 1] - obs_mean) - deviation * shrink) / (total_var * (members - 1.0))
    gain_ref[...] = regroup(gain, lev_index, groups).astype(jnp.bfloat16)
    pad = jnp.zeros((LANES - members, n_obs), jnp.float32)
    dev_all = jnp.concatenate([regroup(deviation, lev_index, groups), pad], axis=0)
    dev_ref[...] = dev_all.T[:, :members].astype(jnp.bfloat16)
    level_all = jnp.concatenate(
        [regroup(level_ref[b], lev_index, groups), jnp.zeros((LANES - lev_rows, n_obs), jnp.float32)], axis=0
    ).T
    for l in range(lev_rows):
        level_b_ref[l] = jnp.broadcast_to(level_all[:, l : l + 1], (n_obs, LANES))
    return obs_mean


def regress(field, shards, l, work):
    _, dev_ref, gain_ref, level_b_ref = work
    members, slab_cols = field.shape
    centred = (field - jnp.sum(field, axis=0, keepdims=True) / members).astype(jnp.bfloat16)
    cross = jnp.dot(dev_ref[...], centred, preferred_element_type=jnp.float32)
    level = jnp.concatenate([level_b_ref[l]] * (slab_cols // LANES), axis=1)
    rows = jnp.concatenate([r[...] for r in shards], axis=0)
    mixed = ((level * rows.astype(jnp.float32)) * cross).astype(jnp.bfloat16)
    return field + jnp.dot(gain_ref[...], mixed, preferred_element_type=jnp.float32)


def first_kernel(groups, sizes, place_ref, frac_ref, cell_ref, own_ref, other_ref, value_ref, var_ref, level_ref, ens_ref, *rest):
    cur_out, mean_ref, keep_ref, send_ref, cur_ref, rows_ref, *work, key_ref, key_smem, list_ref, sems, row_sem, key_sem = rest[groups:]
    shards = [rows_ref, *rest[1:groups]]
    lev_rows = cur_ref.shape[0]
    keys = key_copy(place_ref, cell_ref, key_ref, key_smem, key_sem, sizes)
    keys.start()
    copies = load_levels(ens_ref, cur_ref, sems)
    rows = pltpu.make_async_copy(rest[0].at[0], rows_ref, row_sem)
    rows.start()
    for copy in copies:
        copy.start()
    mean_ref[...] = observe(0, groups, place_ref, own_ref, other_ref, value_ref, var_ref, level_ref, work)
    keys.wait()
    found = list_owned(key_smem, list_ref, 1)
    rows.wait()
    for l in range(lev_rows):
        copies[l].wait()
        cur_out[l] = regress(cur_ref[l], shards, l, work)
    gather_priors(key_smem, frac_ref, list_ref, 1, found, cur_out, work[0])
    split_halves(place_ref[1] & 1, work[0], keep_ref, send_ref)


def last_kernel(groups, place_ref, own_ref, other_ref, value_ref, var_ref, level_ref, mean_in, cur_ref, *rest):
    ens_out, mean_ref, rows_ref, buf_ref, *work, sems, row_sem = rest[groups:]
    shards = [rows_ref, *rest[1:groups]]
    lev_rows = cur_ref.shape[0]
    rows = pltpu.make_async_copy(rest[0].at[1], rows_ref, row_sem)
    rows.start()
    mean_ref[0:1] = mean_in[...]
    mean_ref[1:2] = observe(1, groups, place_ref, own_ref, other_ref, value_ref, var_ref, level_ref, work)
    rows.wait()
    stores = []
    for l in range(lev_rows):
        buf_ref[l] = regress(cur_ref[l], shards, l, work)
        stores.append(pltpu.make_async_copy(buf_ref.at[l], ens_out.at[:, l, :], sems.at[l]))
        stores[l].start()
    for store in stores:
        store.wait()


def with_place(kernel):
    def run(lev_ref, slab_ref, *refs):
        kernel((lev_ref[0], slab_ref[0]), *refs)

    return run


def near(*arrays):
    return [pltpu.with_memory_space_constraint(a, pltpu.VMEM) for a in arrays]


def far(*arrays):
    return [pltpu.with_memory_space_constraint(a, pltpu.HBM) for a in arrays]


def on_device(ensemble, obs_cell, obs_value, obs_var, obs_frac, loc_column, loc_level):
    members, lev_rows, slab_cols = ensemble.shape
    n_blocks, n_obs = obs_cell.shape
    groups = lax.axis_size("lev")
    sizes = (lev_rows, slab_cols, slab_cols * lax.axis_size("slab"))
    place = [lax.axis_index(axis).reshape(1).astype(jnp.int32) for axis in ("lev", "slab")]
    levels = loc_level.transpose(0, 2, 1)

    smem = pl.BlockSpec(memory_space=pltpu.SMEM)
    vmem = pl.BlockSpec(memory_space=pltpu.VMEM)
    hbm = pl.BlockSpec(memory_space=pl.ANY)
    f32 = jnp.float32
    field = pltpu.VMEM((lev_rows, members, slab_cols), f32)
    row = pltpu.VMEM((1, n_obs), f32)
    half = pltpu.VMEM((members, n_obs // 2), f32)
    field_scratch = pltpu.VMEM((lev_rows, members, slab_cols), f32)
    rows_scratch = pltpu.VMEM(loc_column.shape[1:], jnp.bfloat16)
    sum_scratch = pltpu.VMEM((members, n_obs), f32)
    work = [
        sum_scratch,
        pltpu.VMEM((n_obs, members), jnp.bfloat16),
        pltpu.VMEM((members, n_obs), jnp.bfloat16),
        pltpu.VMEM((lev_rows, n_obs, LANES), f32),
    ]
    own = [
        pltpu.VMEM((n_blocks, n_obs), jnp.int32),
        pltpu.SMEM((n_blocks, n_obs), jnp.int32),
        pltpu.SMEM((n_obs + BATCH,), jnp.int32),
    ]
    dma = pltpu.SemaphoreType.DMA((lev_rows,))
    one_dma = pltpu.SemaphoreType.DMA

    shards = [rows_over(loc_column[0], "lev")]

    keep, send = pl.pallas_call(
        with_place(functools.partial(prior_kernel, sizes)),
        out_shape=(half, half),
        in_specs=[smem, smem, smem, vmem, hbm],
        out_specs=(vmem, vmem),
        scratch_shapes=[field_scratch, sum_scratch] + own + [dma, one_dma],
        compiler_params=pltpu.CompilerParams(vmem_limit_bytes=KERNEL_VMEM),
        name="cells",
    )(*place, *far(obs_frac, obs_cell, ensemble))
    later_rows, keep = lax.optimization_barrier((loc_column, keep))
    shards.append(rows_over(later_rows[1], "lev"))
    ours, theirs = add_over(keep, send)

    current, mean_first, keep, send = pl.pallas_call(
        with_place(functools.partial(first_kernel, groups, sizes)),
        out_shape=(field, row, half, half),
        in_specs=[smem, smem, smem] + [vmem] * 6 + [hbm] * 2 + [vmem] * (groups - 1),
        out_specs=(vmem, vmem, vmem, vmem),
        scratch_shapes=[field_scratch, rows_scratch] + work + own + [dma, one_dma, one_dma],
        compiler_params=pltpu.CompilerParams(vmem_limit_bytes=KERNEL_VMEM),
        name="block_first",
    )(*place, obs_frac, obs_cell, *near(ours, theirs), obs_value, obs_var, levels, *far(ensemble, loc_column), *near(*shards[0]))
    ours, theirs = add_over(keep, send)

    analysis, mean = pl.pallas_call(
        with_place(functools.partial(last_kernel, groups)),
        out_shape=(jax.ShapeDtypeStruct(ensemble.shape, f32), jax.ShapeDtypeStruct((n_blocks, n_obs), f32)),
        in_specs=[smem, smem] + [vmem] * 7 + [hbm] + [vmem] * (groups - 1),
        out_specs=(hbm, vmem),
        scratch_shapes=[rows_scratch, field_scratch] + work + [dma, one_dma],
        compiler_params=pltpu.CompilerParams(vmem_limit_bytes=KERNEL_VMEM),
        name="block_last",
    )(*place, *near(ours, theirs), obs_value, obs_var, levels, *near(mean_first, current), *far(loc_column), *near(*shards[1]))
    return (analysis, mean)


def solution(mesh):
    in_specs = (
        P(None, "lev", "slab"),
        P(),
        P(),
        P(),
        P(),
        P(None, "lev", "slab"),
        P(None, None, "lev"),
    )
    out_specs = (P(None, "lev", "slab"), P())
    return jax.shard_map(
        on_device, mesh=mesh, in_specs=in_specs, out_specs=out_specs, check_vma=False
    )
```

```python
import functools

import jax
import jax.numpy as jnp
from jax import lax
from jax.experimental import pallas as pl
from jax.experimental.pallas import tpu as pltpu
from jax.sharding import PartitionSpec as P


LANES = 128
CELL_BITS = 16
BATCH = 4
KERNEL_VMEM = 32 * 1024 * 1024


def swap(value, axis, bit):
    size = lax.axis_size(axis)
    return lax.ppermute(value, axis, [(i, i ^ bit) for i in range(size)])


def rounds_of(axis, first_bit):
    size = lax.axis_size(axis)
    if size & (size - 1):
        raise ValueError("axis size")
    bit = first_bit
    while bit < size:
        if bit * 2 < size:
            yield axis, (bit, bit * 2, bit * 3)
        else:
            yield axis, (bit,)
        bit *= 4


def add_over(keep, send, lev_first):
    half = keep + swap(send, "slab", 1)
    rounds = [list(rounds_of("lev", 1)), list(rounds_of("slab", 2))]
    rounds = sum(rounds if lev_first else rounds[::-1], [])
    for axis, distances in rounds:
        half = sum([swap(half, axis, d) for d in distances], half)
    return half, swap(half, "slab", 1)


def paired_rows(groups):
    return groups == 4


def swap_either(value, even_bit, odd_bit):
    slabs, groups = lax.axis_size("slab"), lax.axis_size("lev")
    pairs = [
        (s * groups + l, s * groups + (l ^ (odd_bit if s & 1 else even_bit)))
        for s in range(slabs)
        for l in range(groups)
    ]
    return lax.ppermute(value, ("slab", "lev"), pairs)


def rows_over(own):
    size = lax.axis_size("lev")
    if paired_rows(size):
        far_even = swap_either(own, 2, 1)
        far_odd = swap_either(own, 1, 2)
        passed = jnp.where((lax.axis_index("slab") & 1) == 0, far_even, far_odd)
        return [far_odd, far_even, swap(passed, "lev", 1)]
    shards = {0: own}
    for p in row_order(size):
        low = p & -p
        shards[p] = swap(shards[p ^ low], "lev", low)
    return [shards[p] for p in range(1, size)]


def row_order(size):
    return sorted(range(1, size), key=lambda p: (bin(p).count("1"), -p))


def key_copy(place_ref, cell_ref, key_ref, key_smem, sem, sizes):
    lev_rows, slab_cols, total_cols = sizes
    lev_index, slab_index = place_ref[0], place_ref[1]
    cell = cell_ref[...]
    edge = slab_index == 0
    lowest = jnp.where(edge, 1, 0)
    key = jnp.full(cell.shape, -1, jnp.int32)
    for r in range(lev_rows):
        col = cell - ((lev_index * lev_rows + r) * total_cols + slab_index * slab_cols - 1)
        key = jnp.where((col >= lowest) & (col <= slab_cols), col + (r << CELL_BITS), key)
        key = jnp.where((col == total_cols) & edge, r << CELL_BITS, key)
    key_ref[...] = key
    return pltpu.make_async_copy(key_ref, key_smem, sem)


def list_owned(key_ref, list_ref, b):
    def step(o, found):
        list_ref[found] = o
        return found + (key_ref[b, o] >= 0).astype(jnp.int32)

    found = lax.fori_loop(0, key_ref.shape[1], step, jnp.int32(0), unroll=16)
    for extra in range(BATCH - 1):
        list_ref[found + extra] = 0
    return found


def gather_priors(key_ref, frac_ref, list_ref, b, found, source_ref, sum_ref):
    members = sum_ref.shape[0]
    slab_cols = source_ref.shape[2]
    lane = lax.broadcasted_iota(jnp.int32, (members, LANES), 1)
    sum_ref[...] = jnp.zeros(sum_ref.shape, jnp.float32)

    def value_of(i):
        o = list_ref[i]
        key = key_ref[b, o]
        fraction = frac_ref[b, o]
        row = jnp.maximum(key, 0) >> CELL_BITS
        col = (jnp.maximum(key, 0) & ((1 << CELL_BITS) - 1)) - 1
        first = jnp.maximum(col, 0)
        second = jnp.minimum(col + 1, slab_cols - 1)
        real = i < found
        weight_first = jnp.where(real & (col >= 0), 1.0 - fraction, 0.0)
        weight_second = jnp.where(real & (col + 1 < slab_cols), fraction, 0.0)
        slot = o & (LANES - 1)

        def picked(c):
            tile = source_ref[row, :, pl.ds(pl.multiple_of((c >> 7) * LANES, LANES), LANES)]
            return pltpu.roll(tile, (slot - c) & (LANES - 1), 1)

        value = weight_first * picked(first) + weight_second * picked(second)
        return (o >> 7) * LANES, jnp.where(lane == slot, value, 0.0)

    def step(i, carry):
        batch = [value_of(i * BATCH + k) for k in range(BATCH)]
        for start, value in batch:
            where_out = pl.ds(pl.multiple_of(start, LANES), LANES)
            sum_ref[:, where_out] = sum_ref[:, where_out] + value
        return carry

    lax.fori_loop(0, (found + BATCH - 1) // BATCH, step, 0)


def half_of(side, width):
    return pl.ds(pl.multiple_of(side * width, LANES), width)


def split_halves(side, sum_ref, keep_ref, send_ref):
    width = keep_ref.shape[1]
    keep_ref[...] = sum_ref[:, half_of(side, width)]
    send_ref[...] = sum_ref[:, half_of(1 - side, width)]


def load_levels(ens_ref, cur_ref, sems):
    return [
        pltpu.make_async_copy(ens_ref.at[:, l, :], cur_ref.at[l], sems.at[l])
        for l in range(cur_ref.shape[0])
    ]


def prior_kernel(sizes, place_ref, frac_ref, cell_ref, ens_ref, keep_ref, send_ref, cur_ref, sum_ref, key_ref, key_smem, list_ref, sems, key_sem):
    copies = load_levels(ens_ref, cur_ref, sems)
    for copy in copies:
        copy.start()
    keys = key_copy(place_ref, cell_ref, key_ref, key_smem, key_sem, sizes)
    keys.start()
    keys.wait()
    found = list_owned(key_smem, list_ref, 0)
    for copy in copies:
        copy.wait()
    gather_priors(key_smem, frac_ref, list_ref, 0, found, cur_ref, sum_ref)
    split_halves(place_ref[1] & 1, sum_ref, keep_ref, send_ref)


def regroup(value, lev_index, side, groups):
    total = value.shape[1]
    block = total // groups
    lane = lax.broadcasted_iota(jnp.int32, value.shape, 1)
    bit = 1
    while bit < groups:
        span = block * bit
        other = jnp.where(
            (lane & span) != 0, pltpu.roll(value, span, 1), pltpu.roll(value, total - span, 1)
        )
        value = jnp.where((lev_index & bit) != 0, other, value)
        bit *= 2
    if paired_rows(groups):
        low, high = pltpu.roll(value, total - block, 1), pltpu.roll(value, block, 1)
        inner = jnp.where(lane < 2 * block, low, high)
        crossed = (side == 1) & (lane >= block) & (lane < 3 * block)
        value = jnp.where(crossed, inner, value)
    return value


def observe(b, groups, place_ref, own_ref, other_ref, value_ref, var_ref, level_ref, work):
    sum_ref, dev_ref, gain_ref, level_b_ref = work
    lev_index, side = place_ref[0], place_ref[1] & 1
    width = own_ref.shape[1]
    sum_ref[:, half_of(side, width)] = own_ref[...]
    sum_ref[:, half_of(1 - side, width)] = other_ref[...]
    prior = sum_ref[...]
    members, n_obs = prior.shape
    lev_rows = level_ref.shape[1]
    variance = var_ref[b : b + 1]
    obs_mean = jnp.sum(prior, axis=0, keepdims=True) / members
    deviation = prior - obs_mean
    spread = jnp.sum(deviation * deviation, axis=0, keepdims=True) / (members - 1.0)
    total_var = spread + variance
    shrink = 1.0 / (1.0 + jnp.sqrt(variance / total_var))
    gain = ((value_ref[b : b + 1] - obs_mean) - deviation * shrink) / (total_var * (members - 1.0))
    gain_ref[...] = regroup(gain, lev_index, side, groups).astype(jnp.bfloat16)
    pad = jnp.zeros((LANES - members, n_obs), jnp.float32)
    dev_all = jnp.concatenate([regroup(deviation, lev_index, side, groups), pad], axis=0)
    dev_ref[...] = dev_all.T[:, :members].astype(jnp.bfloat16)
    level_all = jnp.concatenate(
        [regroup(level_ref[b], lev_index, side, groups), jnp.zeros((LANES - lev_rows, n_obs), jnp.float32)], axis=0
    ).T
    for l in range(lev_rows):
        level_b_ref[l] = jnp.broadcast_to(level_all[:, l : l + 1], (n_obs, LANES))
    return obs_mean


def regress(field, shards, l, work):
    _, dev_ref, gain_ref, level_b_ref = work
    members, slab_cols = field.shape
    centred = (field - jnp.sum(field, axis=0, keepdims=True) / members).astype(jnp.bfloat16)
    cross = jnp.dot(dev_ref[...], centred, preferred_element_type=jnp.float32)
    level = jnp.concatenate([level_b_ref[l]] * (slab_cols // LANES), axis=1)
    rows = jnp.concatenate([r[...] for r in shards], axis=0)
    mixed = ((level * rows.astype(jnp.float32)) * cross).astype(jnp.bfloat16)
    return field + jnp.dot(gain_ref[...], mixed, preferred_element_type=jnp.float32)


def first_kernel(groups, sizes, place_ref, frac_ref, cell_ref, own_ref, other_ref, value_ref, var_ref, level_ref, ens_ref, *rest):
    cur_out, mean_ref, keep_ref, send_ref, cur_ref, rows_ref, *work, key_ref, key_smem, list_ref, sems, row_sem, key_sem = rest[groups:]
    shards = [rows_ref, *rest[1:groups]]
    lev_rows = cur_ref.shape[0]
    keys = key_copy(place_ref, cell_ref, key_ref, key_smem, key_sem, sizes)
    keys.start()
    copies = load_levels(ens_ref, cur_ref, sems)
    rows = pltpu.make_async_copy(rest[0].at[0], rows_ref, row_sem)
    rows.start()
    for copy in copies:
        copy.start()
    mean_ref[...] = observe(0, groups, place_ref, own_ref, other_ref, value_ref, var_ref, level_ref, work)
    keys.wait()
    found = list_owned(key_smem, list_ref, 1)
    rows.wait()
    for l in range(lev_rows):
        copies[l].wait()
        cur_out[l] = regress(cur_ref[l], shards, l, work)
    gather_priors(key_smem, frac_ref, list_ref, 1, found, cur_out, work[0])
    split_halves(place_ref[1] & 1, work[0], keep_ref, send_ref)


def last_kernel(groups, place_ref, own_ref, other_ref, value_ref, var_ref, level_ref, mean_in, cur_ref, *rest):
    ens_out, mean_ref, rows_ref, buf_ref, *work, sems, row_sem = rest[groups:]
    shards = [rows_ref, *rest[1:groups]]
    lev_rows = cur_ref.shape[0]
    rows = pltpu.make_async_copy(rest[0].at[1], rows_ref, row_sem)
    rows.start()
    mean_ref[0:1] = mean_in[...]
    mean_ref[1:2] = observe(1, groups, place_ref, own_ref, other_ref, value_ref, var_ref, level_ref, work)
    rows.wait()
    stores = []
    for l in range(lev_rows):
        buf_ref[l] = regress(cur_ref[l], shards, l, work)
        stores.append(pltpu.make_async_copy(buf_ref.at[l], ens_out.at[:, l, :], sems.at[l]))
        stores[l].start()
    for store in stores:
        store.wait()


def with_place(kernel):
    def run(lev_ref, slab_ref, *refs):
        kernel((lev_ref[0], slab_ref[0]), *refs)

    return run


def near(*arrays):
    return [pltpu.with_memory_space_constraint(a, pltpu.VMEM) for a in arrays]


def far(*arrays):
    return [pltpu.with_memory_space_constraint(a, pltpu.HBM) for a in arrays]


def on_device(ensemble, obs_cell, obs_value, obs_var, obs_frac, loc_column, loc_level):
    members, lev_rows, slab_cols = ensemble.shape
    n_blocks, n_obs = obs_cell.shape
    groups = lax.axis_size("lev")
    sizes = (lev_rows, slab_cols, slab_cols * lax.axis_size("slab"))
    place = [lax.axis_index(axis).reshape(1).astype(jnp.int32) for axis in ("lev", "slab")]
    levels = loc_level.transpose(0, 2, 1)

    smem = pl.BlockSpec(memory_space=pltpu.SMEM)
    vmem = pl.BlockSpec(memory_space=pltpu.VMEM)
    hbm = pl.BlockSpec(memory_space=pl.ANY)
    f32 = jnp.float32
    field = pltpu.VMEM((lev_rows, members, slab_cols), f32)
    row = pltpu.VMEM((1, n_obs), f32)
    half = pltpu.VMEM((members, n_obs // 2), f32)
    field_scratch = pltpu.VMEM((lev_rows, members, slab_cols), f32)
    rows_scratch = pltpu.VMEM(loc_column.shape[1:], jnp.bfloat16)
    sum_scratch = pltpu.VMEM((members, n_obs), f32)
    work = [
        sum_scratch,
        pltpu.VMEM((n_obs, members), jnp.bfloat16),
        pltpu.VMEM((members, n_obs), jnp.bfloat16),
        pltpu.VMEM((lev_rows, n_obs, LANES), f32),
    ]
    own = [
        pltpu.VMEM((n_blocks, n_obs), jnp.int32),
        pltpu.SMEM((n_blocks, n_obs), jnp.int32),
        pltpu.SMEM((n_obs + BATCH,), jnp.int32),
    ]
    dma = pltpu.SemaphoreType.DMA((lev_rows,))
    one_dma = pltpu.SemaphoreType.DMA

    shards = [rows_over(loc_column[0])]

    keep, send = pl.pallas_call(
        with_place(functools.partial(prior_kernel, sizes)),
        out_shape=(half, half),
        in_specs=[smem, smem, smem, vmem, hbm],
        out_specs=(vmem, vmem),
        scratch_shapes=[field_scratch, sum_scratch] + own + [dma, one_dma],
        compiler_params=pltpu.CompilerParams(vmem_limit_bytes=KERNEL_VMEM),
        name="cells",
    )(*place, *far(obs_frac, obs_cell, ensemble))
    later_rows, keep = lax.optimization_barrier((loc_column, keep))
    shards.append(rows_over(later_rows[1]))
    ours, theirs = add_over(keep, send, True)

    current, mean_first, keep, send = pl.pallas_call(
        with_place(functools.partial(first_kernel, groups, sizes)),
        out_shape=(field, row, half, half),
        in_specs=[smem, smem, smem] + [vmem] * 6 + [hbm] * 2 + [vmem] * (groups - 1),
        out_specs=(vmem, vmem, vmem, vmem),
        scratch_shapes=[field_scratch, rows_scratch] + work + own + [dma, one_dma, one_dma],
        compiler_params=pltpu.CompilerParams(vmem_limit_bytes=KERNEL_VMEM),
        name="block_first",
    )(*place, obs_frac, obs_cell, *near(ours, theirs), obs_value, obs_var, levels, *far(ensemble, loc_column), *near(*shards[0]))
    ours, theirs = add_over(keep, send, False)

    analysis, mean = pl.pallas_call(
        with_place(functools.partial(last_kernel, groups)),
        out_shape=(jax.ShapeDtypeStruct(ensemble.shape, f32), jax.ShapeDtypeStruct((n_blocks, n_obs), f32)),
        in_specs=[smem, smem] + [vmem] * 7 + [hbm] + [vmem] * (groups - 1),
        out_specs=(hbm, vmem),
        scratch_shapes=[rows_scratch, field_scratch] + work + [dma, one_dma],
        compiler_params=pltpu.CompilerParams(vmem_limit_bytes=KERNEL_VMEM),
        name="block_last",
    )(*place, *near(ours, theirs), obs_value, obs_var, levels, *near(mean_first, current), *far(loc_column), *near(*shards[1]))
    return (analysis, mean)


def solution(mesh):
    in_specs = (
        P(None, "lev", "slab"),
        P(),
        P(),
        P(),
        P(),
        P(None, "lev", "slab"),
        P(None, None, "lev"),
    )
    out_specs = (P(None, "lev", "slab"), P())
    return jax.shard_map(
        on_device, mesh=mesh, in_specs=in_specs, out_specs=out_specs, check_vma=False
    )
```

```python
import functools

import jax
import jax.numpy as jnp
from jax import lax
from jax.experimental import pallas as pl
from jax.experimental.pallas import tpu as pltpu
from jax.sharding import PartitionSpec as P


LANES = 128
CELL_BITS = 16
BATCH = 4
KERNEL_VMEM = 32 * 1024 * 1024


def swap(value, axis, bit):
    size = lax.axis_size(axis)
    return lax.ppermute(value, axis, [(i, i ^ bit) for i in range(size)])


def rounds_of(axis, first_bit):
    size = lax.axis_size(axis)
    if size & (size - 1):
        raise ValueError("axis size")
    bit = first_bit
    while bit < size:
        if bit * 2 < size:
            yield axis, (bit, bit * 2, bit * 3)
        else:
            yield axis, (bit,)
        bit *= 4


def add_over(keep, send, lev_first):
    half = keep + swap(send, "slab", 1)
    rounds = [list(rounds_of("lev", 1)), list(rounds_of("slab", 2))]
    rounds = sum(rounds if lev_first else rounds[::-1], [])
    for axis, distances in rounds:
        half = sum([swap(half, axis, d) for d in distances], half)
    return half, swap(half, "slab", 1)


def paired_rows(groups):
    return groups == 4


def swap_either(value, even_bit, odd_bit):
    slabs, groups = lax.axis_size("slab"), lax.axis_size("lev")
    bits = [odd_bit if s & 1 else even_bit for s in range(slabs)]
    pairs = [
        (s * groups + l, s * groups + (l ^ bits[s])) for s in range(slabs) for l in range(groups) if bits[s]
    ]
    return lax.ppermute(value, ("slab", "lev"), pairs)


def rows_over(own):
    size = lax.axis_size("lev")
    if paired_rows(size):
        far_even = swap_either(own, 2, 1)
        far_odd = swap_either(own, 1, 2)
        even = (lax.axis_index("slab") & 1) == 0
        on_even = swap_either(far_even, 1, 0)
        on_odd = swap_either(jnp.where(even, own, far_odd), 0, 1)
        return [far_odd, far_even, jnp.where(even, on_even, on_odd)]
    shards = {0: own}
    for p in row_order(size):
        low = p & -p
        shards[p] = swap(shards[p ^ low], "lev", low)
    return [shards[p] for p in range(1, size)]


def row_order(size):
    return sorted(range(1, size), key=lambda p: (bin(p).count("1"), -p))


def key_copy(place_ref, cell_ref, key_ref, key_smem, sem, sizes):
    lev_rows, slab_cols, total_cols = sizes
    lev_index, slab_index = place_ref[0], place_ref[1]
    cell = cell_ref[...]
    edge = slab_index == 0
    lowest = jnp.where(edge, 1, 0)
    key = jnp.full(cell.shape, -1, jnp.int32)
    for r in range(lev_rows):
        col = cell - ((lev_index * lev_rows + r) * total_cols + slab_index * slab_cols - 1)
        key = jnp.where((col >= lowest) & (col <= slab_cols), col + (r << CELL_BITS), key)
        key = jnp.where((col == total_cols) & edge, r << CELL_BITS, key)
    key_ref[...] = key
    return pltpu.make_async_copy(key_ref, key_smem, sem)


def list_owned(key_ref, list_ref, b):
    def step(o, found):
        list_ref[found] = o
        return found + (key_ref[b, o] >= 0).astype(jnp.int32)

    found = lax.fori_loop(0, key_ref.shape[1], step, jnp.int32(0), unroll=16)
    for extra in range(BATCH - 1):
        list_ref[found + extra] = 0
    return found


def gather_priors(key_ref, frac_ref, list_ref, b, found, source_ref, sum_ref):
    members = sum_ref.shape[0]
    slab_cols = source_ref.shape[2]
    lane = lax.broadcasted_iota(jnp.int32, (members, LANES), 1)
    sum_ref[...] = jnp.zeros(sum_ref.shape, jnp.float32)

    def value_of(i):
        o = list_ref[i]
        key = key_ref[b, o]
        fraction = frac_ref[b, o]
        row = jnp.maximum(key, 0) >> CELL_BITS
        col = (jnp.maximum(key, 0) & ((1 << CELL_BITS) - 1)) - 1
        first = jnp.maximum(col, 0)
        second = jnp.minimum(col + 1, slab_cols - 1)
        real = i < found
        weight_first = jnp.where(real & (col >= 0), 1.0 - fraction, 0.0)
        weight_second = jnp.where(real & (col + 1 < slab_cols), fraction, 0.0)
        slot = o & (LANES - 1)

        def picked(c):
            tile = source_ref[row, :, pl.ds(pl.multiple_of((c >> 7) * LANES, LANES), LANES)]
            return pltpu.roll(tile, (slot - c) & (LANES - 1), 1)

        value = weight_first * picked(first) + weight_second * picked(second)
        return (o >> 7) * LANES, jnp.where(lane == slot, value, 0.0)

    def step(i, carry):
        batch = [value_of(i * BATCH + k) for k in range(BATCH)]
        for start, value in batch:
            where_out = pl.ds(pl.multiple_of(start, LANES), LANES)
            sum_ref[:, where_out] = sum_ref[:, where_out] + value
        return carry

    lax.fori_loop(0, (found + BATCH - 1) // BATCH, step, 0)


def half_of(side, width):
    return pl.ds(pl.multiple_of(side * width, LANES), width)


def split_halves(side, sum_ref, keep_ref, send_ref):
    width = keep_ref.shape[1]
    keep_ref[...] = sum_ref[:, half_of(side, width)]
    send_ref[...] = sum_ref[:, half_of(1 - side, width)]


def load_levels(ens_ref, cur_ref, sems):
    return [
        pltpu.make_async_copy(ens_ref.at[:, l, :], cur_ref.at[l], sems.at[l])
        for l in range(cur_ref.shape[0])
    ]


def prior_kernel(sizes, place_ref, frac_ref, cell_ref, ens_ref, keep_ref, send_ref, cur_ref, sum_ref, key_ref, key_smem, list_ref, sems, key_sem):
    copies = load_levels(ens_ref, cur_ref, sems)
    for copy in copies:
        copy.start()
    keys = key_copy(place_ref, cell_ref, key_ref, key_smem, key_sem, sizes)
    keys.start()
    keys.wait()
    found = list_owned(key_smem, list_ref, 0)
    for copy in copies:
        copy.wait()
    gather_priors(key_smem, frac_ref, list_ref, 0, found, cur_ref, sum_ref)
    split_halves(place_ref[1] & 1, sum_ref, keep_ref, send_ref)


def regroup(value, lev_index, side, groups):
    total = value.shape[1]
    block = total // groups
    lane = lax.broadcasted_iota(jnp.int32, value.shape, 1)
    bit = 1
    while bit < groups:
        span = block * bit
        other = jnp.where(
            (lane & span) != 0, pltpu.roll(value, span, 1), pltpu.roll(value, total - span, 1)
        )
        value = jnp.where((lev_index & bit) != 0, other, value)
        bit *= 2
    if paired_rows(groups):
        low, high = pltpu.roll(value, total - block, 1), pltpu.roll(value, block, 1)
        inner = jnp.where(lane < 2 * block, low, high)
        crossed = (side == 1) & (lane >= block) & (lane < 3 * block)
        value = jnp.where(crossed, inner, value)
    return value


def observe(b, groups, place_ref, own_ref, other_ref, value_ref, var_ref, level_ref, work):
    sum_ref, dev_ref, gain_ref, level_b_ref = work
    lev_index, side = place_ref[0], place_ref[1] & 1
    width = own_ref.shape[1]
    sum_ref[:, half_of(side, width)] = own_ref[...]
    sum_ref[:, half_of(1 - side, width)] = other_ref[...]
    prior = sum_ref[...]
    members, n_obs = prior.shape
    lev_rows = level_ref.shape[1]
    variance = var_ref[b : b + 1]
    obs_mean = jnp.sum(prior, axis=0, keepdims=True) / members
    deviation = prior - obs_mean
    spread = jnp.sum(deviation * deviation, axis=0, keepdims=True) / (members - 1.0)
    total_var = spread + variance
    shrink = 1.0 / (1.0 + jnp.sqrt(variance / total_var))
    gain = ((value_ref[b : b + 1] - obs_mean) - deviation * shrink) / (total_var * (members - 1.0))
    gain_ref[...] = regroup(gain, lev_index, side, groups).astype(jnp.bfloat16)
    pad = jnp.zeros((LANES - members, n_obs), jnp.float32)
    dev_all = jnp.concatenate([regroup(deviation, lev_index, side, groups), pad], axis=0)
    dev_ref[...] = dev_all.T[:, :members].astype(jnp.bfloat16)
    level_all = jnp.concatenate(
        [regroup(level_ref[b], lev_index, side, groups), jnp.zeros((LANES - lev_rows, n_obs), jnp.float32)], axis=0
    ).T
    for l in range(lev_rows):
        level_b_ref[l] = jnp.broadcast_to(level_all[:, l : l + 1], (n_obs, LANES))
    return obs_mean


def regress(field, shards, l, work):
    _, dev_ref, gain_ref, level_b_ref = work
    members, slab_cols = field.shape
    centred = (field - jnp.sum(field, axis=0, keepdims=True) / members).astype(jnp.bfloat16)
    cross = jnp.dot(dev_ref[...], centred, preferred_element_type=jnp.float32)
    level = jnp.concatenate([level_b_ref[l]] * (slab_cols // LANES), axis=1)
    rows = jnp.concatenate([r[...] for r in shards], axis=0)
    mixed = ((level * rows.astype(jnp.float32)) * cross).astype(jnp.bfloat16)
    return field + jnp.dot(gain_ref[...], mixed, preferred_element_type=jnp.float32)


def first_kernel(groups, sizes, place_ref, frac_ref, cell_ref, own_ref, other_ref, value_ref, var_ref, level_ref, ens_ref, *rest):
    cur_out, mean_ref, keep_ref, send_ref, cur_ref, rows_ref, *work, key_ref, key_smem, list_ref, sems, row_sem, key_sem = rest[groups:]
    shards = [rows_ref, *rest[1:groups]]
    lev_rows = cur_ref.shape[0]
    keys = key_copy(place_ref, cell_ref, key_ref, key_smem, key_sem, sizes)
    keys.start()
    copies = load_levels(ens_ref, cur_ref, sems)
    rows = pltpu.make_async_copy(rest[0].at[0], rows_ref, row_sem)
    rows.start()
    for copy in copies:
        copy.start()
    mean_ref[...] = observe(0, groups, place_ref, own_ref, other_ref, value_ref, var_ref, level_ref, work)
    keys.wait()
    found = list_owned(key_smem, list_ref, 1)
    rows.wait()
    for l in range(lev_rows):
        copies[l].wait()
        cur_out[l] = regress(cur_ref[l], shards, l, work)
    gather_priors(key_smem, frac_ref, list_ref, 1, found, cur_out, work[0])
    split_halves(place_ref[1] & 1, work[0], keep_ref, send_ref)


def last_kernel(groups, place_ref, own_ref, other_ref, value_ref, var_ref, level_ref, mean_in, cur_ref, *rest):
    ens_out, mean_ref, rows_ref, buf_ref, *work, sems, row_sem = rest[groups:]
    shards = [rows_ref, *rest[1:groups]]
    lev_rows = cur_ref.shape[0]
    rows = pltpu.make_async_copy(rest[0].at[1], rows_ref, row_sem)
    rows.start()
    mean_ref[0:1] = mean_in[...]
    mean_ref[1:2] = observe(1, groups, place_ref, own_ref, other_ref, value_ref, var_ref, level_ref, work)
    rows.wait()
    stores = []
    for l in range(lev_rows):
        buf_ref[l] = regress(cur_ref[l], shards, l, work)
        stores.append(pltpu.make_async_copy(buf_ref.at[l], ens_out.at[:, l, :], sems.at[l]))
        stores[l].start()
    for store in stores:
        store.wait()


def with_place(kernel):
    def run(lev_ref, slab_ref, *refs):
        kernel((lev_ref[0], slab_ref[0]), *refs)

    return run


def near(*arrays):
    return [pltpu.with_memory_space_constraint(a, pltpu.VMEM) for a in arrays]


def far(*arrays):
    return [pltpu.with_memory_space_constraint(a, pltpu.HBM) for a in arrays]


def on_device(ensemble, obs_cell, obs_value, obs_var, obs_frac, loc_column, loc_level):
    members, lev_rows, slab_cols = ensemble.shape
    n_blocks, n_obs = obs_cell.shape
    groups = lax.axis_size("lev")
    sizes = (lev_rows, slab_cols, slab_cols * lax.axis_size("slab"))
    place = [lax.axis_index(axis).reshape(1).astype(jnp.int32) for axis in ("lev", "slab")]
    levels = loc_level.transpose(0, 2, 1)

    smem = pl.BlockSpec(memory_space=pltpu.SMEM)
    vmem = pl.BlockSpec(memory_space=pltpu.VMEM)
    hbm = pl.BlockSpec(memory_space=pl.ANY)
    f32 = jnp.float32
    field = pltpu.VMEM((lev_rows, members, slab_cols), f32)
    row = pltpu.VMEM((1, n_obs), f32)
    half = pltpu.VMEM((members, n_obs // 2), f32)
    field_scratch = pltpu.VMEM((lev_rows, members, slab_cols), f32)
    rows_scratch = pltpu.VMEM(loc_column.shape[1:], jnp.bfloat16)
    sum_scratch = pltpu.VMEM((members, n_obs), f32)
    work = [
        sum_scratch,
        pltpu.VMEM((n_obs, members), jnp.bfloat16),
        pltpu.VMEM((members, n_obs), jnp.bfloat16),
        pltpu.VMEM((lev_rows, n_obs, LANES), f32),
    ]
    own = [
        pltpu.VMEM((n_blocks, n_obs), jnp.int32),
        pltpu.SMEM((n_blocks, n_obs), jnp.int32),
        pltpu.SMEM((n_obs + BATCH,), jnp.int32),
    ]
    dma = pltpu.SemaphoreType.DMA((lev_rows,))
    one_dma = pltpu.SemaphoreType.DMA

    shards = [rows_over(loc_column[0])]

    keep, send = pl.pallas_call(
        with_place(functools.partial(prior_kernel, sizes)),
        out_shape=(half, half),
        in_specs=[smem, smem, smem, vmem, hbm],
        out_specs=(vmem, vmem),
        scratch_shapes=[field_scratch, sum_scratch] + own + [dma, one_dma],
        compiler_params=pltpu.CompilerParams(vmem_limit_bytes=KERNEL_VMEM),
        name="cells",
    )(*place, *far(obs_frac, obs_cell, ensemble))
    later_rows, keep = lax.optimization_barrier((loc_column, keep))
    shards.append(rows_over(later_rows[1]))
    ours, theirs = add_over(keep, send, True)

    current, mean_first, keep, send = pl.pallas_call(
        with_place(functools.partial(first_kernel, groups, sizes)),
        out_shape=(field, row, half, half),
        in_specs=[smem, smem, smem] + [vmem] * 6 + [hbm] * 2 + [vmem] * (groups - 1),
        out_specs=(vmem, vmem, vmem, vmem),
        scratch_shapes=[field_scratch, rows_scratch] + work + own + [dma, one_dma, one_dma],
        compiler_params=pltpu.CompilerParams(vmem_limit_bytes=KERNEL_VMEM),
        name="block_first",
    )(*place, obs_frac, obs_cell, *near(ours, theirs), obs_value, obs_var, levels, *far(ensemble, loc_column), *near(*shards[0]))
    ours, theirs = add_over(keep, send, False)

    analysis, mean = pl.pallas_call(
        with_place(functools.partial(last_kernel, groups)),
        out_shape=(jax.ShapeDtypeStruct(ensemble.shape, f32), jax.ShapeDtypeStruct((n_blocks, n_obs), f32)),
        in_specs=[smem, smem] + [vmem] * 7 + [hbm] + [vmem] * (groups - 1),
        out_specs=(hbm, vmem),
        scratch_shapes=[rows_scratch, field_scratch] + work + [dma, one_dma],
        compiler_params=pltpu.CompilerParams(vmem_limit_bytes=KERNEL_VMEM),
        name="block_last",
    )(*place, *near(ours, theirs), obs_value, obs_var, levels, *near(mean_first, current), *far(loc_column), *near(*shards[1]))
    return (analysis, mean)


def solution(mesh):
    in_specs = (
        P(None, "lev", "slab"),
        P(),
        P(),
        P(),
        P(),
        P(None, "lev", "slab"),
        P(None, None, "lev"),
    )
    out_specs = (P(None, "lev", "slab"), P())
    return jax.shard_map(
        on_device, mesh=mesh, in_specs=in_specs, out_specs=out_specs, check_vma=False
    )
```

```python
import functools

import jax
import jax.numpy as jnp
from jax import lax
from jax.experimental import pallas as pl
from jax.experimental.pallas import tpu as pltpu
from jax.sharding import PartitionSpec as P


LANES = 128
CELL_BITS = 16
BATCH = 4
KERNEL_VMEM = 32 * 1024 * 1024


def swap(value, axis, bit):
    size = lax.axis_size(axis)
    return lax.ppermute(value, axis, [(i, i ^ bit) for i in range(size)])


def rounds_of(axis, first_bit):
    size = lax.axis_size(axis)
    if size & (size - 1):
        raise ValueError("axis size")
    bit = first_bit
    while bit < size:
        if bit * 2 < size:
            yield axis, (bit, bit * 2, bit * 3)
        else:
            yield axis, (bit,)
        bit *= 4


def add_over(keep, send):
    half = keep + swap(send, "slab", 1)
    rounds = list(rounds_of("slab", 2)) + list(rounds_of("lev", 1))
    for axis, distances in rounds:
        half = sum([swap(half, axis, d) for d in distances], half)
    return half, swap(half, "slab", 1)


def paired_rows(groups):
    return groups == 4


def swap_either(value, even_bit, odd_bit):
    slabs, groups = lax.axis_size("slab"), lax.axis_size("lev")
    pairs = [
        (s * groups + l, s * groups + (l ^ (odd_bit if s & 1 else even_bit)))
        for s in range(slabs)
        for l in range(groups)
    ]
    return lax.ppermute(value, ("slab", "lev"), pairs)


def rows_over(own):
    size = lax.axis_size("lev")
    if paired_rows(size):
        far_even = swap_either(own, 2, 1)
        far_odd = swap_either(own, 1, 2)
        passed = jnp.where((lax.axis_index("slab") & 1) == 0, far_even, far_odd)
        return [far_odd, far_even, swap(passed, "lev", 1)]
    shards = {0: own}
    for p in row_order(size):
        low = p & -p
        shards[p] = swap(shards[p ^ low], "lev", low)
    return [shards[p] for p in range(1, size)]


def row_order(size):
    return sorted(range(1, size), key=lambda p: (bin(p).count("1"), -p))


def key_copy(place_ref, cell_ref, key_ref, key_smem, sem, sizes):
    lev_rows, slab_cols, total_cols = sizes
    lev_index, slab_index = place_ref[0], place_ref[1]
    cell = cell_ref[...]
    edge = slab_index == 0
    lowest = jnp.where(edge, 1, 0)
    key = jnp.full(cell.shape, -1, jnp.int32)
    for r in range(lev_rows):
        col = cell - ((lev_index * lev_rows + r) * total_cols + slab_index * slab_cols - 1)
        key = jnp.where((col >= lowest) & (col <= slab_cols), col + (r << CELL_BITS), key)
        key = jnp.where((col == total_cols) & edge, r << CELL_BITS, key)
    key_ref[...] = key
    return pltpu.make_async_copy(key_ref, key_smem, sem)


def list_owned(key_ref, list_ref, b):
    def step(o, found):
        list_ref[found] = o
        return found + (key_ref[b, o] >= 0).astype(jnp.int32)

    found = lax.fori_loop(0, key_ref.shape[1], step, jnp.int32(0), unroll=16)
    for extra in range(BATCH - 1):
        list_ref[found + extra] = 0
    return found


def gather_priors(key_ref, frac_ref, list_ref, b, found, source_ref, sum_ref):
    members = sum_ref.shape[0]
    slab_cols = source_ref.shape[2]
    lane = lax.broadcasted_iota(jnp.int32, (members, LANES), 1)
    sum_ref[...] = jnp.zeros(sum_ref.shape, jnp.float32)

    def value_of(i):
        o = list_ref[i]
        key = key_ref[b, o]
        fraction = frac_ref[b, o]
        row = jnp.maximum(key, 0) >> CELL_BITS
        col = (jnp.maximum(key, 0) & ((1 << CELL_BITS) - 1)) - 1
        first = jnp.maximum(col, 0)
        second = jnp.minimum(col + 1, slab_cols - 1)
        real = i < found
        weight_first = jnp.where(real & (col >= 0), 1.0 - fraction, 0.0)
        weight_second = jnp.where(real & (col + 1 < slab_cols), fraction, 0.0)
        slot = o & (LANES - 1)

        def picked(c):
            tile = source_ref[row, :, pl.ds(pl.multiple_of((c >> 7) * LANES, LANES), LANES)]
            return pltpu.roll(tile, (slot - c) & (LANES - 1), 1)

        value = weight_first * picked(first) + weight_second * picked(second)
        return (o >> 7) * LANES, jnp.where(lane == slot, value, 0.0)

    def step(i, carry):
        batch = [value_of(i * BATCH + k) for k in range(BATCH)]
        for start, value in batch:
            where_out = pl.ds(pl.multiple_of(start, LANES), LANES)
            sum_ref[:, where_out] = sum_ref[:, where_out] + value
        return carry

    lax.fori_loop(0, (found + BATCH - 1) // BATCH, step, 0)


def half_of(side, width):
    return pl.ds(pl.multiple_of(side * width, LANES), width)


def split_halves(side, sum_ref, keep_ref, send_ref):
    width = keep_ref.shape[1]
    keep_ref[...] = sum_ref[:, half_of(side, width)]
    send_ref[...] = sum_ref[:, half_of(1 - side, width)]


def load_levels(ens_ref, cur_ref, sems):
    return [
        pltpu.make_async_copy(ens_ref.at[:, l, :], cur_ref.at[l], sems.at[l])
        for l in range(cur_ref.shape[0])
    ]


def prior_kernel(sizes, place_ref, frac_ref, cell_ref, ens_ref, keep_ref, send_ref, cur_ref, sum_ref, key_ref, key_smem, list_ref, sems, key_sem):
    copies = load_levels(ens_ref, cur_ref, sems)
    for copy in copies:
        copy.start()
    keys = key_copy(place_ref, cell_ref, key_ref, key_smem, key_sem, sizes)
    keys.start()
    keys.wait()
    found = list_owned(key_smem, list_ref, 0)
    for copy in copies:
        copy.wait()
    gather_priors(key_smem, frac_ref, list_ref, 0, found, cur_ref, sum_ref)
    split_halves(place_ref[1] & 1, sum_ref, keep_ref, send_ref)


def regroup(value, lev_index, side, groups):
    total = value.shape[1]
    block = total // groups
    lane = lax.broadcasted_iota(jnp.int32, value.shape, 1)
    bit = 1
    while bit < groups:
        span = block * bit
        other = jnp.where(
            (lane & span) != 0, pltpu.roll(value, span, 1), pltpu.roll(value, total - span, 1)
        )
        value = jnp.where((lev_index & bit) != 0, other, value)
        bit *= 2
    if paired_rows(groups):
        low, high = pltpu.roll(value, total - block, 1), pltpu.roll(value, block, 1)
        inner = jnp.where(lane < 2 * block, low, high)
        crossed = (side == 1) & (lane >= block) & (lane < 3 * block)
        value = jnp.where(crossed, inner, value)
    return value


def observe(b, groups, place_ref, own_ref, other_ref, value_ref, var_ref, level_ref, work):
    sum_ref, dev_ref, gain_ref, level_b_ref = work
    lev_index, side = place_ref[0], place_ref[1] & 1
    width = own_ref.shape[1]
    sum_ref[:, half_of(side, width)] = own_ref[...]
    sum_ref[:, half_of(1 - side, width)] = other_ref[...]
    prior = sum_ref[...]
    members, n_obs = prior.shape
    lev_rows = level_ref.shape[1]
    variance = var_ref[b : b + 1]
    obs_mean = jnp.sum(prior, axis=0, keepdims=True) / members
    deviation = prior - obs_mean
    spread = jnp.sum(deviation * deviation, axis=0, keepdims=True) / (members - 1.0)
    total_var = spread + variance
    shrink = 1.0 / (1.0 + jnp.sqrt(variance / total_var))
    gain = ((value_ref[b : b + 1] - obs_mean) - deviation * shrink) / (total_var * (members - 1.0))
    gain_ref[...] = regroup(gain, lev_index, side, groups).astype(jnp.bfloat16)
    pad = jnp.zeros((LANES - members, n_obs), jnp.float32)
    dev_all = jnp.concatenate([regroup(deviation, lev_index, side, groups), pad], axis=0)
    dev_ref[...] = dev_all.T[:, :members].astype(jnp.bfloat16)
    level_all = jnp.concatenate(
        [regroup(level_ref[b], lev_index, side, groups), jnp.zeros((LANES - lev_rows, n_obs), jnp.float32)], axis=0
    ).T
    for l in range(lev_rows):
        level_b_ref[l] = jnp.broadcast_to(level_all[:, l : l + 1], (n_obs, LANES))
    return obs_mean


def regress(field, shards, l, work):
    _, dev_ref, gain_ref, level_b_ref = work
    members, slab_cols = field.shape
    centred = (field - jnp.sum(field, axis=0, keepdims=True) / members).astype(jnp.bfloat16)
    cross = jnp.dot(dev_ref[...], centred, preferred_element_type=jnp.float32)
    level = jnp.concatenate([level_b_ref[l]] * (slab_cols // LANES), axis=1)
    rows = jnp.concatenate([r[...] for r in shards], axis=0)
    mixed = ((level * rows.astype(jnp.float32)) * cross).astype(jnp.bfloat16)
    return field + jnp.dot(gain_ref[...], mixed, preferred_element_type=jnp.float32)


def first_kernel(groups, sizes, place_ref, frac_ref, cell_ref, own_ref, other_ref, value_ref, var_ref, level_ref, ens_ref, *rest):
    cur_out, mean_ref, keep_ref, send_ref, cur_ref, rows_ref, *work, key_ref, key_smem, list_ref, sems, row_sem, key_sem = rest[groups:]
    shards = [rows_ref, *rest[1:groups]]
    lev_rows = cur_ref.shape[0]
    keys = key_copy(place_ref, cell_ref, key_ref, key_smem, key_sem, sizes)
    keys.start()
    copies = load_levels(ens_ref, cur_ref, sems)
    rows = pltpu.make_async_copy(rest[0].at[0], rows_ref, row_sem)
    rows.start()
    for copy in copies:
        copy.start()
    mean_ref[...] = observe(0, groups, place_ref, own_ref, other_ref, value_ref, var_ref, level_ref, work)
    keys.wait()
    found = list_owned(key_smem, list_ref, 1)
    rows.wait()
    for l in range(lev_rows):
        copies[l].wait()
        cur_out[l] = regress(cur_ref[l], shards, l, work)
    gather_priors(key_smem, frac_ref, list_ref, 1, found, cur_out, work[0])
    split_halves(place_ref[1] & 1, work[0], keep_ref, send_ref)


def last_kernel(groups, place_ref, own_ref, other_ref, value_ref, var_ref, level_ref, mean_in, cur_ref, *rest):
    ens_out, mean_ref, rows_ref, buf_ref, *work, sems, row_sem = rest[groups:]
    shards = [rows_ref, *rest[1:groups]]
    lev_rows = cur_ref.shape[0]
    rows = pltpu.make_async_copy(rest[0].at[1], rows_ref, row_sem)
    rows.start()
    mean_ref[0:1] = mean_in[...]
    mean_ref[1:2] = observe(1, groups, place_ref, own_ref, other_ref, value_ref, var_ref, level_ref, work)
    rows.wait()
    stores = []
    for l in range(lev_rows):
        buf_ref[l] = regress(cur_ref[l], shards, l, work)
        stores.append(pltpu.make_async_copy(buf_ref.at[l], ens_out.at[:, l, :], sems.at[l]))
        stores[l].start()
    for store in stores:
        store.wait()


def with_place(kernel):
    def run(lev_ref, slab_ref, *refs):
        kernel((lev_ref[0], slab_ref[0]), *refs)

    return run


def near(*arrays):
    return [pltpu.with_memory_space_constraint(a, pltpu.VMEM) for a in arrays]


def far(*arrays):
    return [pltpu.with_memory_space_constraint(a, pltpu.HBM) for a in arrays]


def on_device(ensemble, obs_cell, obs_value, obs_var, obs_frac, loc_column, loc_level):
    members, lev_rows, slab_cols = ensemble.shape
    n_blocks, n_obs = obs_cell.shape
    groups = lax.axis_size("lev")
    sizes = (lev_rows, slab_cols, slab_cols * lax.axis_size("slab"))
    place = [lax.axis_index(axis).reshape(1).astype(jnp.int32) for axis in ("lev", "slab")]
    levels = loc_level.transpose(0, 2, 1)

    smem = pl.BlockSpec(memory_space=pltpu.SMEM)
    vmem = pl.BlockSpec(memory_space=pltpu.VMEM)
    hbm = pl.BlockSpec(memory_space=pl.ANY)
    f32 = jnp.float32
    field = pltpu.VMEM((lev_rows, members, slab_cols), f32)
    row = pltpu.VMEM((1, n_obs), f32)
    half = pltpu.VMEM((members, n_obs // 2), f32)
    field_scratch = pltpu.VMEM((lev_rows, members, slab_cols), f32)
    rows_scratch = pltpu.VMEM(loc_column.shape[1:], jnp.bfloat16)
    sum_scratch = pltpu.VMEM((members, n_obs), f32)
    work = [
        sum_scratch,
        pltpu.VMEM((n_obs, members), jnp.bfloat16),
        pltpu.VMEM((members, n_obs), jnp.bfloat16),
        pltpu.VMEM((lev_rows, n_obs, LANES), f32),
    ]
    own = [
        pltpu.VMEM((n_blocks, n_obs), jnp.int32),
        pltpu.SMEM((n_blocks, n_obs), jnp.int32),
        pltpu.SMEM((n_obs + BATCH,), jnp.int32),
    ]
    dma = pltpu.SemaphoreType.DMA((lev_rows,))
    one_dma = pltpu.SemaphoreType.DMA

    shards = [rows_over(loc_column[0])]

    keep, send = pl.pallas_call(
        with_place(functools.partial(prior_kernel, sizes)),
        out_shape=(half, half),
        in_specs=[smem, smem, smem, vmem, hbm],
        out_specs=(vmem, vmem),
        scratch_shapes=[field_scratch, sum_scratch] + own + [dma, one_dma],
        compiler_params=pltpu.CompilerParams(vmem_limit_bytes=KERNEL_VMEM),
        name="cells",
    )(*place, *far(obs_frac, obs_cell, ensemble))
    later_rows, keep = lax.optimization_barrier((loc_column, keep))
    shards.append(rows_over(later_rows[1]))
    ours, theirs = add_over(keep, send)

    current, mean_first, keep, send = pl.pallas_call(
        with_place(functools.partial(first_kernel, groups, sizes)),
        out_shape=(field, row, half, half),
        in_specs=[smem, smem, smem] + [vmem] * 6 + [hbm] * 2 + [vmem] * (groups - 1),
        out_specs=(vmem, vmem, vmem, vmem),
        scratch_shapes=[field_scratch, rows_scratch] + work + own + [dma, one_dma, one_dma],
        compiler_params=pltpu.CompilerParams(vmem_limit_bytes=KERNEL_VMEM),
        name="block_first",
    )(*place, obs_frac, obs_cell, *near(ours, theirs), obs_value, obs_var, levels, *far(ensemble, loc_column), *near(*shards[0]))
    ours, theirs = add_over(keep, send)

    analysis, mean = pl.pallas_call(
        with_place(functools.partial(last_kernel, groups)),
        out_shape=(jax.ShapeDtypeStruct(ensemble.shape, f32), jax.ShapeDtypeStruct((n_blocks, n_obs), f32)),
        in_specs=[smem, smem] + [vmem] * 7 + [hbm] + [vmem] * (groups - 1),
        out_specs=(hbm, vmem),
        scratch_shapes=[rows_scratch, field_scratch] + work + [dma, one_dma],
        compiler_params=pltpu.CompilerParams(vmem_limit_bytes=KERNEL_VMEM),
        name="block_last",
    )(*place, *near(ours, theirs), obs_value, obs_var, levels, *near(mean_first, current), *far(loc_column), *near(*shards[1]))
    return (analysis, mean)


def solution(mesh):
    in_specs = (
        P(None, "lev", "slab"),
        P(),
        P(),
        P(),
        P(),
        P(None, "lev", "slab"),
        P(None, None, "lev"),
    )
    out_specs = (P(None, "lev", "slab"), P())
    return jax.shard_map(
        on_device, mesh=mesh, in_specs=in_specs, out_specs=out_specs, check_vma=False
    )
```

```python
import functools

import jax
import jax.numpy as jnp
from jax import lax
from jax.experimental import pallas as pl
from jax.experimental.pallas import tpu as pltpu
from jax.sharding import PartitionSpec as P


LANES = 128
CELL_BITS = 16
BATCH = 4
KERNEL_VMEM = 32 * 1024 * 1024


def swap(value, axis, bit):
    size = lax.axis_size(axis)
    return lax.ppermute(value, axis, [(i, i ^ bit) for i in range(size)])


def rounds_of(axis, first_bit):
    size = lax.axis_size(axis)
    if size & (size - 1):
        raise ValueError("axis size")
    bit = first_bit
    while bit < size:
        if bit * 2 < size:
            yield axis, (bit, bit * 2, bit * 3)
        else:
            yield axis, (bit,)
        bit *= 4


def add_over(keep, send):
    half = keep + swap(send, "slab", 1)
    rounds = list(rounds_of("lev", 1)) + list(rounds_of("slab", 2))
    for axis, distances in rounds:
        half = sum([swap(half, axis, d) for d in distances], half)
    return half, swap(half, "slab", 1)


def paired_rows(groups, b):
    return groups == 4 and b == 0


def swap_either(value, even_bit, odd_bit):
    slabs, groups = lax.axis_size("slab"), lax.axis_size("lev")
    pairs = [
        (s * groups + l, s * groups + (l ^ (odd_bit if s & 1 else even_bit)))
        for s in range(slabs)
        for l in range(groups)
    ]
    return lax.ppermute(value, ("slab", "lev"), pairs)


def rows_over(own, b):
    size = lax.axis_size("lev")
    if paired_rows(size, b):
        far_even = swap_either(own, 2, 1)
        far_odd = swap_either(own, 1, 2)
        passed = jnp.where((lax.axis_index("slab") & 1) == 0, far_even, far_odd)
        return [far_odd, far_even, swap(passed, "lev", 1)]
    shards = {0: own}
    for p in row_order(size):
        low = p & -p
        shards[p] = swap(shards[p ^ low], "lev", low)
    return [shards[p] for p in range(1, size)]


def row_order(size):
    return sorted(range(1, size), key=lambda p: (bin(p).count("1"), -p))


def key_copy(place_ref, cell_ref, key_ref, key_smem, sem, sizes):
    lev_rows, slab_cols, total_cols = sizes
    lev_index, slab_index = place_ref[0], place_ref[1]
    cell = cell_ref[...]
    edge = slab_index == 0
    lowest = jnp.where(edge, 1, 0)
    key = jnp.full(cell.shape, -1, jnp.int32)
    for r in range(lev_rows):
        col = cell - ((lev_index * lev_rows + r) * total_cols + slab_index * slab_cols - 1)
        key = jnp.where((col >= lowest) & (col <= slab_cols), col + (r << CELL_BITS), key)
        key = jnp.where((col == total_cols) & edge, r << CELL_BITS, key)
    key_ref[...] = key
    return pltpu.make_async_copy(key_ref, key_smem, sem)


def list_owned(key_ref, list_ref, b):
    def step(o, found):
        list_ref[found] = o
        return found + (key_ref[b, o] >= 0).astype(jnp.int32)

    found = lax.fori_loop(0, key_ref.shape[1], step, jnp.int32(0), unroll=16)
    for extra in range(BATCH - 1):
        list_ref[found + extra] = 0
    return found


def gather_priors(key_ref, frac_ref, list_ref, b, found, source_ref, sum_ref):
    members = sum_ref.shape[0]
    slab_cols = source_ref.shape[2]
    lane = lax.broadcasted_iota(jnp.int32, (members, LANES), 1)
    sum_ref[...] = jnp.zeros(sum_ref.shape, jnp.float32)

    def value_of(i):
        o = list_ref[i]
        key = key_ref[b, o]
        fraction = frac_ref[b, o]
        row = jnp.maximum(key, 0) >> CELL_BITS
        col = (jnp.maximum(key, 0) & ((1 << CELL_BITS) - 1)) - 1
        first = jnp.maximum(col, 0)
        second = jnp.minimum(col + 1, slab_cols - 1)
        real = i < found
        weight_first = jnp.where(real & (col >= 0), 1.0 - fraction, 0.0)
        weight_second = jnp.where(real & (col + 1 < slab_cols), fraction, 0.0)
        slot = o & (LANES - 1)

        def picked(c):
            tile = source_ref[row, :, pl.ds(pl.multiple_of((c >> 7) * LANES, LANES), LANES)]
            return pltpu.roll(tile, (slot - c) & (LANES - 1), 1)

        value = weight_first * picked(first) + weight_second * picked(second)
        return (o >> 7) * LANES, jnp.where(lane == slot, value, 0.0)

    def step(i, carry):
        batch = [value_of(i * BATCH + k) for k in range(BATCH)]
        for start, value in batch:
            where_out = pl.ds(pl.multiple_of(start, LANES), LANES)
            sum_ref[:, where_out] = sum_ref[:, where_out] + value
        return carry

    lax.fori_loop(0, (found + BATCH - 1) // BATCH, step, 0)


def half_of(side, width):
    return pl.ds(pl.multiple_of(side * width, LANES), width)


def split_halves(side, sum_ref, keep_ref, send_ref):
    width = keep_ref.shape[1]
    keep_ref[...] = sum_ref[:, half_of(side, width)]
    send_ref[...] = sum_ref[:, half_of(1 - side, width)]


def load_levels(ens_ref, cur_ref, sems):
    return [
        pltpu.make_async_copy(ens_ref.at[:, l, :], cur_ref.at[l], sems.at[l])
        for l in range(cur_ref.shape[0])
    ]


def prior_kernel(sizes, place_ref, frac_ref, cell_ref, ens_ref, keep_ref, send_ref, cur_ref, sum_ref, key_ref, key_smem, list_ref, sems, key_sem):
    copies = load_levels(ens_ref, cur_ref, sems)
    for copy in copies:
        copy.start()
    keys = key_copy(place_ref, cell_ref, key_ref, key_smem, key_sem, sizes)
    keys.start()
    keys.wait()
    found = list_owned(key_smem, list_ref, 0)
    for copy in copies:
        copy.wait()
    gather_priors(key_smem, frac_ref, list_ref, 0, found, cur_ref, sum_ref)
    split_halves(place_ref[1] & 1, sum_ref, keep_ref, send_ref)


def regroup(value, lev_index, side, groups, b):
    total = value.shape[1]
    block = total // groups
    lane = lax.broadcasted_iota(jnp.int32, value.shape, 1)
    bit = 1
    while bit < groups:
        span = block * bit
        other = jnp.where(
            (lane & span) != 0, pltpu.roll(value, span, 1), pltpu.roll(value, total - span, 1)
        )
        value = jnp.where((lev_index & bit) != 0, other, value)
        bit *= 2
    if paired_rows(groups, b):
        low, high = pltpu.roll(value, total - block, 1), pltpu.roll(value, block, 1)
        inner = jnp.where(lane < 2 * block, low, high)
        crossed = (side == 1) & (lane >= block) & (lane < 3 * block)
        value = jnp.where(crossed, inner, value)
    return value


def observe(b, groups, place_ref, own_ref, other_ref, value_ref, var_ref, level_ref, work):
    sum_ref, dev_ref, gain_ref, level_b_ref = work
    lev_index, side = place_ref[0], place_ref[1] & 1
    width = own_ref.shape[1]
    sum_ref[:, half_of(side, width)] = own_ref[...]
    sum_ref[:, half_of(1 - side, width)] = other_ref[...]
    prior = sum_ref[...]
    members, n_obs = prior.shape
    lev_rows = level_ref.shape[1]
    variance = var_ref[b : b + 1]
    obs_mean = jnp.sum(prior, axis=0, keepdims=True) / members
    deviation = prior - obs_mean
    spread = jnp.sum(deviation * deviation, axis=0, keepdims=True) / (members - 1.0)
    total_var = spread + variance
    shrink = 1.0 / (1.0 + jnp.sqrt(variance / total_var))
    gain = ((value_ref[b : b + 1] - obs_mean) - deviation * shrink) / (total_var * (members - 1.0))
    gain_ref[...] = regroup(gain, lev_index, side, groups, b).astype(jnp.bfloat16)
    pad = jnp.zeros((LANES - members, n_obs), jnp.float32)
    dev_all = jnp.concatenate([regroup(deviation, lev_index, side, groups, b), pad], axis=0)
    dev_ref[...] = dev_all.T[:, :members].astype(jnp.bfloat16)
    level_all = jnp.concatenate(
        [regroup(level_ref[b], lev_index, side, groups, b), jnp.zeros((LANES - lev_rows, n_obs), jnp.float32)], axis=0
    ).T
    for l in range(lev_rows):
        level_b_ref[l] = jnp.broadcast_to(level_all[:, l : l + 1], (n_obs, LANES))
    return obs_mean


def regress(field, shards, l, work):
    _, dev_ref, gain_ref, level_b_ref = work
    members, slab_cols = field.shape
    centred = (field - jnp.sum(field, axis=0, keepdims=True) / members).astype(jnp.bfloat16)
    cross = jnp.dot(dev_ref[...], centred, preferred_element_type=jnp.float32)
    level = jnp.concatenate([level_b_ref[l]] * (slab_cols // LANES), axis=1)
    rows = jnp.concatenate([r[...] for r in shards], axis=0)
    mixed = ((level * rows.astype(jnp.float32)) * cross).astype(jnp.bfloat16)
    return field + jnp.dot(gain_ref[...], mixed, preferred_element_type=jnp.float32)


def first_kernel(groups, sizes, place_ref, frac_ref, cell_ref, own_ref, other_ref, value_ref, var_ref, level_ref, ens_ref, *rest):
    cur_out, mean_ref, keep_ref, send_ref, cur_ref, rows_ref, *work, key_ref, key_smem, list_ref, sems, row_sem, key_sem = rest[groups:]
    shards = [rows_ref, *rest[1:groups]]
    lev_rows = cur_ref.shape[0]
    keys = key_copy(place_ref, cell_ref, key_ref, key_smem, key_sem, sizes)
    keys.start()
    copies = load_levels(ens_ref, cur_ref, sems)
    rows = pltpu.make_async_copy(rest[0].at[0], rows_ref, row_sem)
    rows.start()
    for copy in copies:
        copy.start()
    mean_ref[...] = observe(0, groups, place_ref, own_ref, other_ref, value_ref, var_ref, level_ref, work)
    keys.wait()
    found = list_owned(key_smem, list_ref, 1)
    rows.wait()
    for l in range(lev_rows):
        copies[l].wait()
        cur_out[l] = regress(cur_ref[l], shards, l, work)
    gather_priors(key_smem, frac_ref, list_ref, 1, found, cur_out, work[0])
    split_halves(place_ref[1] & 1, work[0], keep_ref, send_ref)


def last_kernel(groups, place_ref, own_ref, other_ref, value_ref, var_ref, level_ref, mean_in, cur_ref, *rest):
    ens_out, mean_ref, rows_ref, buf_ref, *work, sems, row_sem = rest[groups:]
    shards = [rows_ref, *rest[1:groups]]
    lev_rows = cur_ref.shape[0]
    rows = pltpu.make_async_copy(rest[0].at[1], rows_ref, row_sem)
    rows.start()
    mean_ref[0:1] = mean_in[...]
    mean_ref[1:2] = observe(1, groups, place_ref, own_ref, other_ref, value_ref, var_ref, level_ref, work)
    rows.wait()
    stores = []
    for l in range(lev_rows):
        buf_ref[l] = regress(cur_ref[l], shards, l, work)
        stores.append(pltpu.make_async_copy(buf_ref.at[l], ens_out.at[:, l, :], sems.at[l]))
        stores[l].start()
    for store in stores:
        store.wait()


def with_place(kernel):
    def run(lev_ref, slab_ref, *refs):
        kernel((lev_ref[0], slab_ref[0]), *refs)

    return run


def near(*arrays):
    return [pltpu.with_memory_space_constraint(a, pltpu.VMEM) for a in arrays]


def far(*arrays):
    return [pltpu.with_memory_space_constraint(a, pltpu.HBM) for a in arrays]


def on_device(ensemble, obs_cell, obs_value, obs_var, obs_frac, loc_column, loc_level):
    members, lev_rows, slab_cols = ensemble.shape
    n_blocks, n_obs = obs_cell.shape
    groups = lax.axis_size("lev")
    sizes = (lev_rows, slab_cols, slab_cols * lax.axis_size("slab"))
    place = [lax.axis_index(axis).reshape(1).astype(jnp.int32) for axis in ("lev", "slab")]
    levels = loc_level.transpose(0, 2, 1)

    smem = pl.BlockSpec(memory_space=pltpu.SMEM)
    vmem = pl.BlockSpec(memory_space=pltpu.VMEM)
    hbm = pl.BlockSpec(memory_space=pl.ANY)
    f32 = jnp.float32
    field = pltpu.VMEM((lev_rows, members, slab_cols), f32)
    row = pltpu.VMEM((1, n_obs), f32)
    half = pltpu.VMEM((members, n_obs // 2), f32)
    field_scratch = pltpu.VMEM((lev_rows, members, slab_cols), f32)
    rows_scratch = pltpu.VMEM(loc_column.shape[1:], jnp.bfloat16)
    sum_scratch = pltpu.VMEM((members, n_obs), f32)
    work = [
        sum_scratch,
        pltpu.VMEM((n_obs, members), jnp.bfloat16),
        pltpu.VMEM((members, n_obs), jnp.bfloat16),
        pltpu.VMEM((lev_rows, n_obs, LANES), f32),
    ]
    own = [
        pltpu.VMEM((n_blocks, n_obs), jnp.int32),
        pltpu.SMEM((n_blocks, n_obs), jnp.int32),
        pltpu.SMEM((n_obs + BATCH,), jnp.int32),
    ]
    dma = pltpu.SemaphoreType.DMA((lev_rows,))
    one_dma = pltpu.SemaphoreType.DMA

    shards = [rows_over(loc_column[0], 0)]

    keep, send = pl.pallas_call(
        with_place(functools.partial(prior_kernel, sizes)),
        out_shape=(half, half),
        in_specs=[smem, smem, smem, vmem, hbm],
        out_specs=(vmem, vmem),
        scratch_shapes=[field_scratch, sum_scratch] + own + [dma, one_dma],
        compiler_params=pltpu.CompilerParams(vmem_limit_bytes=KERNEL_VMEM),
        name="cells",
    )(*place, *far(obs_frac, obs_cell, ensemble))
    later_rows, keep = lax.optimization_barrier((loc_column, keep))
    shards.append(rows_over(later_rows[1], 1))
    ours, theirs = add_over(keep, send)

    current, mean_first, keep, send = pl.pallas_call(
        with_place(functools.partial(first_kernel, groups, sizes)),
        out_shape=(field, row, half, half),
        in_specs=[smem, smem, smem] + [vmem] * 6 + [hbm] * 2 + [vmem] * (groups - 1),
        out_specs=(vmem, vmem, vmem, vmem),
        scratch_shapes=[field_scratch, rows_scratch] + work + own + [dma, one_dma, one_dma],
        compiler_params=pltpu.CompilerParams(vmem_limit_bytes=KERNEL_VMEM),
        name="block_first",
    )(*place, obs_frac, obs_cell, *near(ours, theirs), obs_value, obs_var, levels, *far(ensemble, loc_column), *near(*shards[0]))
    ours, theirs = add_over(keep, send)

    analysis, mean = pl.pallas_call(
        with_place(functools.partial(last_kernel, groups)),
        out_shape=(jax.ShapeDtypeStruct(ensemble.shape, f32), jax.ShapeDtypeStruct((n_blocks, n_obs), f32)),
        in_specs=[smem, smem] + [vmem] * 7 + [hbm] + [vmem] * (groups - 1),
        out_specs=(hbm, vmem),
        scratch_shapes=[rows_scratch, field_scratch] + work + [dma, one_dma],
        compiler_params=pltpu.CompilerParams(vmem_limit_bytes=KERNEL_VMEM),
        name="block_last",
    )(*place, *near(ours, theirs), obs_value, obs_var, levels, *near(mean_first, current), *far(loc_column), *near(*shards[1]))
    return (analysis, mean)


def solution(mesh):
    in_specs = (
        P(None, "lev", "slab"),
        P(),
        P(),
        P(),
        P(),
        P(None, "lev", "slab"),
        P(None, None, "lev"),
    )
    out_specs = (P(None, "lev", "slab"), P())
    return jax.shard_map(
        on_device, mesh=mesh, in_specs=in_specs, out_specs=out_specs, check_vma=False
    )
```
